32 devices in a mesh: gx: 4 (over z), gy: 8 (over y, x, core).
Axes of the slice: x: 2, y: 2, z: 4, core: 2. Of those that a mesh axis runs over, the one named last changes fastest.
Arguments:
- tables: float32 [2, 262144, 128], P(None, ('gx', 'gy')), may hold values from -0.9 to 0.9
- cold_rows: int32 [32, 2, 32, 16], P(('gx', 'gy')), may hold values from 0 to 8191, as said below
- cold_bags: int32 [32, 2, 32, 16], P(('gx', 'gy')), may hold values from -1 to 127, as said below
- hot_rows: int32 [2, 256], replicated, may hold values from 0 to 262143
- hot_ids: int32 [4096, 2, 8], P(('gx', 'gy')), may hold values from 0 to 255
Outputs:
- pooled: float32 [4096, 2, 128], P(('gx', 'gy'))
The draws below stay inside these ranges and needn't reach their ends.
Inputs may be any that keep to these rules, and one draw needn't show every extreme that they name: `cold_rows`: every entry names one of the owner's 8192 rows. `cold_bags`: live slots of one sender, table and owner come first, the empty ones (-1) after them; in every draw each table has an owner whose 16 slots are all live from every sender.
All inputs are finite; a program needn't handle non-finite values.
Results may differ from the reference program's by a relative error of at most 0.0003.
Values sent between devices are 32-bit elements; how exact they have to be, the bound alone decides.
A program may use at most 64 MiB of HBM per device.

```python
import jax
import jax.numpy as jnp
from jax import lax

DIM = 128
ROWS_DEV = 8192
TABLES = 2
BATCH_DEV = 128
CAP = 16
HOT = 256
HOT_BAG = 8
PEERS = 32
BATCH = 4096
ROWS = 262144


def draw_cold_rows(key, part):
    shape_all = (PEERS, TABLES, PEERS, CAP)
    exponent = jax.random.randint(jax.random.fold_in(key, 101), shape_all, 0, 21)
    limit = jnp.minimum(jnp.left_shift(jnp.ones(shape_all, jnp.int32), exponent), ROWS_DEV)
    return jax.random.randint(jax.random.fold_in(key, 102), shape_all, 0, limit).astype(jnp.int32)


def draw_cold_bags(key, part):
    shape_all = (PEERS, TABLES, PEERS, CAP)
    busiest = jax.random.randint(jax.random.fold_in(key, 201), (TABLES,), 0, PEERS)
    filled = jax.random.randint(jax.random.fold_in(key, 202), (PEERS, TABLES, PEERS), max(1, CAP // 4), CAP + 1)
    owner_index = jnp.arange(PEERS, dtype=jnp.int32)[None, None, :]
    filled = jnp.where(owner_index == busiest[None, :, None], CAP, filled)
    samples = jax.random.randint(jax.random.fold_in(key, 203), shape_all, 0, BATCH_DEV)
    slot_index = jnp.arange(CAP, dtype=jnp.int32)
    return jnp.where(slot_index < filled[..., None], samples, -1).astype(jnp.int32)


def place_ends(entries, rng, smallest, largest):
    longest = entries.shape.index(max(entries.shape))
    spots = []
    for shift in (0, 1):
        where = [jax.random.randint(jax.random.fold_in(rng, axis), (), 0, length) for axis, length in enumerate(entries.shape)]
        where[longest] = (where[longest] + shift) % entries.shape[longest]
        spots.append(tuple(where))
    return entries.at[spots[0]].set(smallest).at[spots[1]].set(largest)


def shard_levels(own_key, extent, pieces, least, high):
    def one(position, parts):
        draws = jax.random.uniform(jax.random.fold_in(jax.random.fold_in(own_key, 6), position), (parts,), jnp.float32, least / len(pieces), high / len(pieces))
        return jnp.repeat(jnp.exp(draws), extent[position] // parts).reshape((-1,) + (1,) * (len(extent) - position - 1))

    gain = one(*pieces[0])
    for cut in pieces[1:]:
        gain = gain * one(*cut)
    return gain


def centred(stream_key, shape, deviation, reach, cuts=(), kind=jnp.bfloat16):
    drawn = jax.random.normal(stream_key, shape, jnp.float32) * deviation
    if len(cuts) > 0:
        drawn = shard_levels(stream_key, shape, cuts, -0.22, 0.18) * drawn
    return jnp.clip(drawn, min=-reach, max=reach).astype(kind)


def setup_inputs(seed: int = 0) -> dict:
    key_list = jax.random.split(jax.random.key(seed), 6)
    return {
        "tables": centred(key_list[0], (TABLES, ROWS, DIM), 0.15, 0.9, ((1, 32),), jnp.float32),
        "cold_rows": draw_cold_rows(jax.random.fold_in(key_list[5], 71), 0),
        "cold_bags": draw_cold_bags(jax.random.fold_in(key_list[5], 71), 0),
        "hot_rows": place_ends(jax.random.randint(key_list[3], (TABLES, HOT), 0, ROWS), jax.random.fold_in(key_list[3], 1), 0, ROWS - 1).astype(jnp.int32),
        "hot_ids": place_ends(jax.random.randint(key_list[4], (BATCH, TABLES, HOT_BAG), 0, HOT), jax.random.fold_in(key_list[4], 1), 0, HOT - 1).astype(jnp.int32),
    }


def take_rows(matrix, indices):
    return jnp.take(matrix, indices, axis=0)


def reference(tables, cold_rows, cold_bags, hot_rows, hot_ids):
    offsets = (jnp.arange(PEERS, dtype=jnp.int32) * ROWS_DEV)[:, None]

    def per_table(table_index):
        one_table = tables[table_index]

        def per_sender(sender):
            slot_rows = (cold_rows[sender, table_index] + offsets).reshape(-1)
            slot_bags = cold_bags[sender, table_index].reshape(-1)
            looked = take_rows(one_table, slot_rows)
            live_mask = slot_bags >= 0
            segment = jnp.where(live_mask, slot_bags, 0).astype(jnp.int32)
            values = jnp.where(live_mask[:, None], looked, jnp.zeros_like(looked))
            return jax.ops.segment_sum(values, segment, num_segments=BATCH_DEV)

        return lax.map(per_sender, jnp.arange(PEERS, dtype=jnp.int32))

    cold_part = lax.map(per_table, jnp.arange(TABLES, dtype=jnp.int32))
    cold_part = jnp.transpose(cold_part, (1, 2, 0, 3)).reshape(BATCH, TABLES, DIM)
    hot_table = jax.vmap(take_rows)(tables, hot_rows)

    def pool_hot(table_rows, lookups):
        return jnp.sum(take_rows(table_rows, lookups), axis=1)

    hot_part = jax.vmap(pool_hot, in_axes=(0, 1), out_axes=1)(hot_table, hot_ids)
    return cold_part + hot_part
```

```python
import functools
import math

import jax
import jax.numpy as jnp
from jax import lax
from jax.experimental import pallas as pl
from jax.experimental.pallas import tpu as pltpu
from jax.sharding import PartitionSpec as P

MESH = pl.DeviceIdType.MESH
CHUNKS = 4
EARLY = 0.0


def ORDER(i, nx, ny):
    return i // ny, lax.rem(i, ny)


def split2(x):
    hi = x.astype(jnp.bfloat16)
    return hi, (x - hi.astype(jnp.float32)).astype(jnp.bfloat16)


def pool(weights, values):
    hi, lo = split2(values)
    return jnp.dot(weights, hi, preferred_element_type=jnp.float32) + jnp.dot(
        weights, lo, preferred_element_type=jnp.float32
    )


def kernel(nx, ny, tables_ref, rows_hbm, bags_hbm, hot_rows_hbm, hot_ids_hbm, out_ref,
           tab, rows_ref, bags_ref, hot_rows_ref, hot_ids_ref,
           idx_out, idx_s, stage, recv, hot_stage, hot_in, hot_part, hot_z, hot_tab,
           onehot, counts, tab_sem, in_sem, idx_send, idx_recv, idx_local, cold_send, cold_recv,
           hot_send, hot_recv, z_send, z_recv, gat_send, gat_recv):
    peers = nx * ny
    half = nx // 2
    tcount, rows_dev, width = tab.shape
    cap = rows_ref.shape[1]
    hot = hot_rows_ref.shape[1]
    chunk = hot_tab.shape[0] // ny
    batch = out_ref.shape[0] // tcount
    gx, gy = lax.axis_index("gx"), lax.axis_index("gy")
    me = gx * ny + gy

    def peer(i):
        m, j = ORDER(i, nx, ny)
        px = lax.rem(gx // half + 1 + m // half, 2) * half + lax.rem(gx + m, half)
        py = lax.rem(gy + j, ny)
        return px, py, px * ny + py

    def others(fn):
        def step(i, carry):
            px, py, p = peer(i)

            @pl.when(p != me)
            def _():
                fn(px, py, p)
            return carry
        lax.fori_loop(0, peers, step, 0)

    def plane_others(fn):
        def step(j, carry):
            fn(lax.rem(gy + j, ny))
            return carry
        lax.fori_loop(1, ny, step, 0)

    small = []
    for n, (src, dst) in enumerate(((rows_hbm, rows_ref), (hot_rows_hbm, hot_rows_ref),
                                    (bags_hbm, bags_ref), (hot_ids_hbm, hot_ids_ref))):
        load = pltpu.make_async_copy(src, dst, in_sem.at[n])
        load.start()
        small.append(load)

    piece = rows_dev // CHUNKS
    loads = []
    for t in range(tcount):
        for c in range(CHUNKS):
            part = pl.ds(c * piece, piece)
            load = pltpu.make_async_copy(tables_ref.at[t, part], tab.at[t, part], tab_sem.at[t, c])
            load.start()
            loads.append(load)

    barrier = pltpu.get_barrier_semaphore()
    others(lambda px, py, p: pl.semaphore_signal(
        barrier, inc=1, device_id=(px, py), device_id_type=MESH))

    small[0].wait()
    lines = rows_ref[...].reshape(tcount * cap, peers).T
    for p in range(peers):
        idx_out[p, :, 0:tcount * cap] = lines[p:p + 1, :]
    pl.semaphore_wait(barrier, peers - 1)

    own_idx = pltpu.make_async_copy(idx_out.at[me], idx_s.at[me], idx_local)
    own_idx.start()

    def send_idx(px, py, p):
        pltpu.make_async_remote_copy(
            src_ref=idx_out.at[p], dst_ref=idx_s.at[me], send_sem=idx_send, recv_sem=idx_recv,
            device_id=(px, py), device_id_type=MESH).start()
    others(send_idx)

    small[1].wait()
    for load in loads:
        load.wait()

    base = me * rows_dev
    group = math.gcd(chunk, 16)

    def pick_hot(y):
        def rows_of(g, carry):
            start = y * chunk + g * group
            t = start // hot
            first = start - t * hot
            for j in range(group):
                local = hot_rows_ref[t, first + j] - base
                mine = jnp.logical_and(local >= 0, local < rows_dev).astype(jnp.float32)
                at = jnp.clip(local, 0, rows_dev - 1)
                hot_stage[y, pl.ds(g * group + j, 1), :] = tab[t, pl.ds(at, 1), :] * mine
            return carry
        lax.fori_loop(0, chunk // group, rows_of, 0)

    def send_hot(y):
        pltpu.make_async_remote_copy(
            src_ref=hot_stage.at[y], dst_ref=hot_in.at[gy], send_sem=hot_send, recv_sem=hot_recv,
            device_id=(gx, y), device_id_type=MESH).start()

    def hot_step(j, carry):
        pick_hot(lax.rem(gy + j, ny))

        @pl.when(j > 1)
        def _():
            send_hot(lax.rem(gy + j - 1, ny))
        return carry
    lax.fori_loop(1, ny + 1, hot_step, 0)
    hot_in[gy] = hot_stage[gy]

    some = pl.ds(0, peers - 1)
    pltpu.make_async_copy(idx_s.at[some], idx_s.at[some], idx_recv).wait()
    own_idx.wait()

    def pick(p):
        for t in range(tcount):
            for c in range(cap):
                k = t * cap + c
                stage[p, k:k + 1, :] = tab[t, pl.ds(idx_s[p, 0, k], 1), :]

    def send_cold(i):
        px, py, p = peer(i)

        @pl.when(p != me)
        def _():
            pltpu.make_async_remote_copy(
                src_ref=stage.at[p], dst_ref=recv.at[me], send_sem=cold_send, recv_sem=cold_recv,
                device_id=(px, py), device_id_type=MESH).start()

    def cold_steps(first, last):
        def step(i, carry):
            pick(peer(i)[2])

            @pl.when(i > 0)
            def _():
                send_cold(i - 1)
            return carry
        lax.fori_loop(first, last, step, 0)

    early = int(peers * EARLY)
    cold_steps(0, early)

    planes = pl.ds(0, ny - 1)
    pltpu.make_async_copy(hot_in.at[planes], hot_in.at[planes], hot_recv).wait()
    hot_part[...] = jnp.sum(hot_in[...], axis=0)
    hot_z[gx] = hot_part[...]
    cold_steps(early, early + 1)

    def send_z(k, carry):
        pltpu.make_async_remote_copy(
            src_ref=hot_part, dst_ref=hot_z.at[gx], send_sem=z_send, recv_sem=z_recv,
            device_id=(lax.rem(gx + k, nx), gy), device_id_type=MESH).start()
        return carry
    lax.fori_loop(1, nx, send_z, 0)
    cold_steps(early + 1, peers)
    recv[me] = stage[me]
    small[2].wait()
    small[3].wait()
    send_cold(peers - 1)

    slots = peers * cap
    owner = lax.broadcasted_iota(jnp.int32, (peers, slots), 1) // cap
    spread = (owner == lax.broadcasted_iota(jnp.int32, (peers, slots), 0)).astype(jnp.float32)
    place = lax.rem(lax.broadcasted_iota(jnp.int32, (cap, slots), 1), cap)
    mask = place == lax.broadcasted_iota(jnp.int32, (cap, slots), 0)
    samples = lax.broadcasted_iota(jnp.int32, (batch, slots), 0).astype(jnp.float32)

    def cold_weights(t):
        wide = jnp.dot(bags_ref[t].astype(jnp.float32), spread,
                       precision=lax.Precision.HIGHEST, preferred_element_type=jnp.float32)
        flat = jnp.sum(jnp.where(mask, wide, 0.0), axis=0, keepdims=True)
        onehot[t] = (flat == samples).astype(jnp.bfloat16)

    cold_weights(0)

    zs = pl.ds(0, nx - 1)
    pltpu.make_async_copy(hot_z.at[zs], hot_z.at[zs], z_recv).wait()
    mine_at = pl.ds(pl.multiple_of(gy * chunk, chunk), chunk)
    hot_tab[mine_at, :] = jnp.sum(hot_z[...], axis=0)
    for t in range(1, tcount):
        cold_weights(t)

    def send_gat(y):
        pltpu.make_async_remote_copy(
            src_ref=hot_tab.at[mine_at], dst_ref=hot_tab.at[mine_at], send_sem=gat_send,
            recv_sem=gat_recv, device_id=(gx, y), device_id_type=MESH).start()
    plane_others(send_gat)

    entry = lax.broadcasted_iota(jnp.int32, (hot, batch), 0)
    for t in range(tcount):
        total = jnp.zeros((hot, batch), jnp.float32)
        for k in range(hot_ids_ref.shape[1]):
            total += (hot_ids_ref[t, k:k + 1, :] == entry).astype(jnp.float32)
        counts[t] = total.T.astype(jnp.bfloat16)

    rest = pl.ds(0, (ny - 1) * chunk)

    def pool_cold():
        pltpu.make_async_copy(recv.at[some], recv.at[some], cold_recv).wait()
        return [pool(onehot[t], recv[:, t * cap:(t + 1) * cap, :].reshape(slots, width))
                for t in range(tcount)]

    def pool_hot():
        pltpu.make_async_copy(hot_tab.at[rest], hot_tab.at[rest], gat_recv).wait()
        return [pool(counts[t], hot_tab[t * hot:(t + 1) * hot, :]) for t in range(tcount)]

    for t, part in enumerate(pool_cold()):
        out_ref[t::tcount, :] = part
    for t, part in enumerate(pool_hot()):
        out_ref[t::tcount, :] += part

    pltpu.make_async_copy(idx_out.at[some], idx_out.at[some], idx_send).wait()
    pltpu.make_async_copy(hot_stage.at[planes], hot_stage.at[planes], hot_send).wait()
    pltpu.make_async_copy(stage.at[some], stage.at[some], cold_send).wait()
    pltpu.make_async_copy(hot_z.at[zs], hot_z.at[zs], z_send).wait()
    pltpu.make_async_copy(hot_tab.at[rest], hot_tab.at[rest], gat_send).wait()


def solution(mesh):
    nx, ny = mesh.shape["gx"], mesh.shape["gy"]
    peers = nx * ny

    def body(tables, cold_rows, cold_bags, hot_rows, hot_ids):
        tcount, rows_dev, width = tables.shape
        cap = cold_rows.shape[3]
        batch = hot_ids.shape[0]
        hot = hot_rows.shape[1]
        chunk = tcount * hot // ny
        assert nx % 2 == 0 and chunk * ny == tcount * hot and hot % math.gcd(chunk, 16) == 0
        lanes = -(-tcount * cap // 128) * 128
        rows_t = jnp.transpose(cold_rows[0], (0, 2, 1))
        bags_t = jnp.transpose(cold_bags[0], (0, 2, 1))
        ids_t = jnp.transpose(hot_ids, (1, 2, 0))
        hbm = pl.BlockSpec(memory_space=pltpu.HBM)
        out = pl.pallas_call(
            functools.partial(kernel, nx, ny),
            out_shape=pltpu.VMEM((batch * tcount, width), jnp.float32),
            in_specs=[hbm] * 5,
            out_specs=pl.BlockSpec(memory_space=pltpu.VMEM),
            scratch_shapes=[
                pltpu.VMEM((tcount, rows_dev, width), jnp.float32),
                pltpu.VMEM(rows_t.shape, jnp.int32),
                pltpu.VMEM(bags_t.shape, jnp.int32),
                pltpu.SMEM(hot_rows.shape, jnp.int32),
                pltpu.VMEM(ids_t.shape, jnp.int32),
                pltpu.VMEM((peers, 1, lanes), jnp.int32),
                pltpu.SMEM((peers, 1, lanes), jnp.int32),
                pltpu.VMEM((peers, tcount * cap, width), jnp.float32),
                pltpu.VMEM((peers, tcount * cap, width), jnp.float32),
                pltpu.VMEM((ny, chunk, width), jnp.float32),
                pltpu.VMEM((ny, chunk, width), jnp.float32),
                pltpu.VMEM((chunk, width), jnp.float32),
                pltpu.VMEM((nx, chunk, width), jnp.float32),
                pltpu.VMEM((tcount * hot, width), jnp.float32),
                pltpu.VMEM((tcount, batch, peers * cap), jnp.bfloat16),
                pltpu.VMEM((tcount, batch, hot), jnp.bfloat16),
                pltpu.SemaphoreType.DMA((tcount, CHUNKS)),
                pltpu.SemaphoreType.DMA((4,)),
            ] + [pltpu.SemaphoreType.DMA] * 11,
            compiler_params=pltpu.CompilerParams(
                collective_id=0, has_side_effects=True, vmem_limit_bytes=67043328 - 131072),
        )(tables, rows_t, bags_t, hot_rows, ids_t)
        return out.reshape(batch, tcount, width)

    return jax.shard_map(
        body,
        mesh=mesh,
        in_specs=(
            P(None, ("gx", "gy"), None),
            P(("gx", "gy"), None, None, None),
            P(("gx", "gy"), None, None, None),
            P(),
            P(("gx", "gy"), None, None),
        ),
        out_specs=P(("gx", "gy"), None, None),
        check_vma=False,
    )
```

```python
import functools
import math

import jax
import jax.numpy as jnp
from jax import lax
from jax.experimental import pallas as pl
from jax.experimental.pallas import tpu as pltpu
from jax.sharding import PartitionSpec as P

MESH = pl.DeviceIdType.MESH
CHUNKS = 4
PAD = 8
VMEM_BYTES = 67043328


def split2(x):
    hi = x.astype(jnp.bfloat16)
    return hi, (x - hi.astype(jnp.float32)).astype(jnp.bfloat16)


def pool(weights, values):
    hi, lo = split2(values)
    return jnp.dot(weights, hi, preferred_element_type=jnp.float32) + jnp.dot(
        weights, lo, preferred_element_type=jnp.float32
    )


def plane_order(nx, u):
    rest = [q for q in range(nx) if q not in (u, u + 1)]
    return [u + 1, u] + sorted(rest, key=lambda q: (abs(q - u), q < u))


def kernel(nx, ny, tables_ref, rows_hbm, bags_hbm, hot_rows_hbm, hot_ids_hbm, out_ref,
           rows_ref, bags_ref, hot_rows_ref, hot_at, hot_ids_ref,
           idx_out, idx_s, stage, recv, hot_stage, pair_in, hot_in, hot_sum, hot_z, hot_tab,
           onehot, counts, tab_sem, in_sem, hot_at_sem, idx_send, idx_recv, idx_local,
           cold_send, cold_recv, pair_send, pair_recv, hot_send, hot_recv, z_send, z_recv,
           gat_send, gat_recv, fwd_send, fwd_recv, *tabs):
    peers = nx * ny
    half, chips = nx // 2, ny // 2
    tcount, rows_dev, width = tables_ref.shape
    cap = rows_ref.shape[1]
    hot = hot_rows_ref.shape[1]
    chunk = hot_tab.shape[0] // chips
    batch = out_ref.shape[0] // tcount
    gx, gy = lax.axis_index("gx"), lax.axis_index("gy")
    me = gx * ny + gy
    chip, core = gy // 2, lax.rem(gy, 2)
    partner = gy + 1 - 2 * core
    hub = core == 1
    low = gx < half
    u = jnp.where(low, gx, nx - 1 - gx)

    orders = [plane_order(nx, k) for k in range(half)]
    px_of = []
    for m in range(nx):
        q = jnp.int32(orders[0][m])
        for k in range(1, half):
            q = jnp.where(u == k, orders[k][m], q)
        px_of.append(jnp.where(low, q, nx - 1 - q))

    def flip(v, n, j):
        y, b = 0, 1
        while b < n:
            y += lax.rem(v // b + j // b, 2) * b
            b *= 2
        return y

    py_of = [flip(gy, ny, j) for j in range(ny)]

    def span_of(m, first, last):
        return range(max(first, 1) if m == 1 else first, last)

    def remote(src, dst, send_sem, recv_sem, px, py):
        return pltpu.make_async_remote_copy(
            src_ref=src, dst_ref=dst, send_sem=send_sem, recv_sem=recv_sem,
            device_id=(px, py), device_id_type=MESH)

    small = [pltpu.make_async_copy(src, dst, in_sem.at[n]) for n, (src, dst) in enumerate(
        ((rows_hbm, rows_ref), (hot_rows_hbm, hot_rows_ref),
         (bags_hbm, bags_ref), (hot_ids_hbm, hot_ids_ref)))]
    piece = rows_dev // CHUNKS
    loads = []
    for t in range(tcount):
        for c in range(CHUNKS):
            part = pl.ds(c * piece, piece)
            loads.append(pltpu.make_async_copy(
                tables_ref.at[t, part], tabs[t].at[part], tab_sem.at[t, c]))
    small[0].start()
    small[1].start()

    barrier = pltpu.get_barrier_semaphore()
    for m in reversed(range(nx)):
        for j in span_of(m, 0, ny):
            pl.semaphore_signal(
                barrier, inc=1, device_id=(px_of[m], py_of[j]), device_id_type=MESH)

    for load in loads:
        load.start()
    small[2].start()
    small[3].start()
    for t in range(tcount):
        tabs[t][rows_dev:rows_dev + PAD, :] = jnp.zeros((PAD, width), jnp.float32)

    small[1].wait()
    local = hot_rows_ref[...] - me * rows_dev
    hot_rows_ref[...] = jnp.where(
        jnp.logical_and(local >= 0, local < rows_dev), local, rows_dev)
    small[0].wait()
    where_hot = pltpu.make_async_copy(hot_rows_ref, hot_at, hot_at_sem)
    where_hot.start()
    lines = rows_ref[...].reshape(tcount * cap, peers).T
    for p in range(peers):
        idx_out[p, :, 0:tcount * cap] = lines[p:p + 1, :]
    own_idx = pltpu.make_async_copy(idx_out.at[me], idx_s.at[me], idx_local)
    own_idx.start()

    group = math.gcd(hot, 32)

    def pick_hot(t):
        def step(g, carry):
            for j in range(group):
                hot_stage[pl.ds(t * hot + g * group + j, 1), :] = tabs[t][
                    pl.ds(hot_at[t, g * group + j], 1), :]
            return carry
        lax.fori_loop(0, hot // group, step, 0)

    def pick_hot_when(t):
        for load in loads[t * CHUNKS:(t + 1) * CHUNKS]:
            load.wait()
        pick_hot(t)

    where_hot.wait()
    pick_hot_when(0)
    pl.semaphore_wait(barrier, peers - 1)
    for m in range(nx):
        for j in span_of(m, 0, ny):
            remote(idx_out.at[px_of[m] * ny + py_of[j]], idx_s.at[me], idx_send, idx_recv.at[me],
                   px_of[m], py_of[j]).start()
    for t in range(1, tcount):
        pick_hot_when(t)

    def rows_of(y):
        return pl.ds(pl.multiple_of(y * chunk, chunk), chunk)

    def take(m, first, last):
        def step(j, carry):
            p = px_of[m] * ny + flip(gy, ny, j)
            pltpu.make_async_copy(idx_s.at[p], idx_s.at[p], idx_recv.at[p]).wait()
            pick(p)
            return carry
        span = span_of(m, first, last)
        lax.fori_loop(span.start, span.stop, step, 0)

    def pick(p):
        for t in range(tcount):
            for c in range(cap):
                k = t * cap + c
                stage[p, k:k + 1, :] = tabs[t][pl.ds(idx_s[p, 0, k], 1), :]

    def send(m, first, last):
        for j in span_of(m, first, last):
            remote(stage.at[px_of[m] * ny + py_of[j]], recv.at[me], cold_send, cold_recv.at[gx],
                   px_of[m], py_of[j]).start()

    def pair_sends(t):
        rows = pl.ds(t * hot, hot)
        remote(hot_stage.at[rows], pair_in.at[rows], pair_send.at[t], pair_recv.at[t],
               gx, partner).start()

    def pair_sum():
        for t in range(tcount):
            rows = pl.ds(t * hot, hot)
            pltpu.make_async_copy(
                pair_in.at[rows], pair_in.at[rows], pair_recv.at[t]).wait()
            pair_in[rows, :] = pair_in[rows, :] + hot_stage[rows, :]

    def hot_sends():
        for k in range(1, chips):
            to = flip(chip, chips, k)
            remote(pair_in.at[rows_of(to)], hot_in.at[chip], hot_send, hot_recv,
                   gx, 2 * to + core).start()
        hot_in[chip] = pair_in[rows_of(chip), :]

    others = pl.ds(0, chips - 1)

    def hot_reduce():
        pltpu.make_async_copy(hot_in.at[others], hot_in.at[others], hot_recv).wait()
        hot_sum[0] = jnp.sum(hot_in[...], axis=0)

    levels = nx.bit_length() - 1

    def z_send_to(k):
        b = 1 << k
        to = gx + b - 2 * b * lax.rem(gx // b, 2)
        remote(hot_sum.at[k], hot_z.at[k], z_send.at[k], z_recv.at[k], to, gy).start()

    def z_sum(k):
        pltpu.make_async_copy(hot_z.at[k], hot_z.at[k], z_recv.at[k]).wait()
        total = hot_sum[k] + hot_z[k]
        if k + 1 < levels:
            hot_sum[k + 1] = total
        else:
            hot_tab[rows_of(chip), :] = total

    def gat_sends():
        mine = hot_tab.at[rows_of(chip)]
        for k in range(1, chips):
            remote(mine, mine, gat_send, gat_recv.at[k], gx,
                   2 * flip(chip, chips, k) + core).start()
        remote(mine, mine, fwd_send, fwd_recv, gx, partner).start()

    def forward():
        for k in range(1, chips):
            got = hot_tab.at[rows_of(flip(chip, chips, k))]
            pltpu.make_async_copy(got, got, gat_recv.at[k]).wait()
            remote(got, got, fwd_send, fwd_recv, gx, partner).start()

    slots = peers * cap
    owner = lax.broadcasted_iota(jnp.int32, (peers, slots), 1) // cap
    spread = (owner == lax.broadcasted_iota(jnp.int32, (peers, slots), 0)).astype(jnp.float32)
    place = lax.rem(lax.broadcasted_iota(jnp.int32, (cap, slots), 1), cap)
    mask = place == lax.broadcasted_iota(jnp.int32, (cap, slots), 0)
    samples = lax.broadcasted_iota(jnp.int32, (batch, slots), 0).astype(jnp.float32)

    def cold_weights(t):
        wide = jnp.dot(bags_ref[t].astype(jnp.float32), spread,
                       precision=lax.Precision.HIGHEST, preferred_element_type=jnp.float32)
        flat = jnp.sum(jnp.where(mask, wide, 0.0), axis=0, keepdims=True)
        onehot[t] = (flat == samples).astype(jnp.bfloat16)

    entry = lax.broadcasted_iota(jnp.int32, (hot, batch), 0)

    def hot_counts(t):
        total = jnp.zeros((hot, batch), jnp.float32)
        for k in range(hot_ids_ref.shape[1]):
            total += (hot_ids_ref[t, k:k + 1, :] == entry).astype(jnp.float32)
        counts[t] = total.T.astype(jnp.bfloat16)

    @pl.when(hub)
    def _():
        for m in (0, *range(3, nx)):
            take(m, 0, 2)
            send(m, 0, 2)
        pair_sum()
        take(1, 0, ny // 2)
        hot_sends()
        take(2, 0, 2)
        send(2, 0, 2)
        take(1, ny // 2, ny)
        take(0, 2, ny)
        for m in range(2, nx):
            take(m, 2, ny)
        own_idx.wait()
        pick(me)
        hot_reduce()
        recv[me] = stage[me]
        send(1, 0, ny)
        z_send_to(0)
        small[2].wait()
        small[3].wait()
        cold_weights(0)
        z_sum(0)
        hot_counts(0)
        for k in range(1, levels):
            z_send_to(k)
            if k == levels - 1:
                for m in (0, *range(2, nx)):
                    send(m, 2, ny)
                for t in range(1, tcount):
                    hot_counts(t)
            z_sum(k)
        for t in range(1, tcount):
            cold_weights(t)
        gat_sends()

    @pl.when(jnp.logical_not(hub))
    def _():
        for t in range(tcount):
            pair_sends(t)
        for m in (0, *range(3, nx), 2):
            take(m, 0, 2)
            send(m, 0, 2)
        for m in (0, *range(3, nx), 2):
            take(m, 2, ny)
            send(m, 2, ny)
        take(1, 0, ny)
        own_idx.wait()
        pick(me)
        send(1, 0, ny)
        recv[me] = stage[me]
        small[2].wait()
        small[3].wait()
        for t in range(tcount):
            hot_counts(t)
            cold_weights(t)


    @pl.when(hub)
    def _():
        forward()

    sums = [jnp.zeros((batch, width), jnp.float32) for _ in range(tcount)]

    def pool_plane(m):
        count = pl.ds(0, ny - 1 if m == 1 else ny)
        pltpu.make_async_copy(recv.at[count], recv.at[count], cold_recv.at[px_of[m]]).wait()
        at = pl.ds(pl.multiple_of(px_of[m] * ny, ny), ny)
        cols = pl.ds(pl.multiple_of(px_of[m] * ny * cap, ny * cap), ny * cap)
        for t in range(tcount):
            values = recv[at, t * cap:(t + 1) * cap, :].reshape(ny * cap, width)
            sums[t] = sums[t] + pool(onehot[t, :, cols], values)

    pool_plane(1)
    @pl.when(jnp.logical_not(hub))
    def _():
        pltpu.make_async_copy(hot_tab, hot_tab, fwd_recv).wait()

    for t in range(tcount):
        sums[t] = sums[t] + pool(counts[t], hot_tab[t * hot:(t + 1) * hot, :])
    for m in (0, *range(2, nx)):
        pool_plane(m)
    for t in range(tcount):
        out_ref[t::tcount, :] = sums[t]

    some = pl.ds(0, peers - 1)
    pltpu.make_async_copy(idx_out.at[some], idx_out.at[some], idx_send).wait()
    pltpu.make_async_copy(stage.at[some], stage.at[some], cold_send).wait()

    @pl.when(jnp.logical_not(hub))
    def _():
        for t in range(tcount):
            rows = pl.ds(t * hot, hot)
            pltpu.make_async_copy(hot_stage.at[rows], hot_stage.at[rows], pair_send.at[t]).wait()

    @pl.when(hub)
    def _():
        pltpu.make_async_copy(hot_in.at[others], hot_in.at[others], hot_send).wait()
        for k in range(levels):
            pltpu.make_async_copy(hot_sum.at[k], hot_sum.at[k], z_send.at[k]).wait()
        apart = pl.ds(0, (chips - 1) * chunk)
        pltpu.make_async_copy(hot_tab.at[apart], hot_tab.at[apart], gat_send).wait()
        pltpu.make_async_copy(hot_tab, hot_tab, fwd_send).wait()


def solution(mesh):
    nx, ny = mesh.shape["gx"], mesh.shape["gy"]
    peers = nx * ny

    def body(tables, cold_rows, cold_bags, hot_rows, hot_ids):
        tcount, rows_dev, width = tables.shape
        cap = cold_rows.shape[3]
        batch = hot_ids.shape[0]
        hot = hot_rows.shape[1]
        chunk = tcount * hot // (ny // 2)
        levels = nx.bit_length() - 1
        assert nx == 1 << levels and ny & (ny - 1) == 0 and min(nx, ny) > 1
        assert chunk * (ny // 2) == tcount * hot and chunk % 8 == 0 and ny * cap % 128 == 0
        lanes = -(-tcount * cap // 128) * 128
        rows_t = jnp.transpose(cold_rows[0], (0, 2, 1))
        bags_t = jnp.transpose(cold_bags[0], (0, 2, 1))
        ids_t = jnp.transpose(hot_ids, (1, 2, 0))
        hbm = pl.BlockSpec(memory_space=pltpu.HBM)
        out = pl.pallas_call(
            functools.partial(kernel, nx, ny),
            out_shape=pltpu.VMEM((batch * tcount, width), jnp.float32),
            in_specs=[hbm] * 5,
            out_specs=pl.BlockSpec(memory_space=pltpu.VMEM),
            scratch_shapes=[
                pltpu.VMEM(rows_t.shape, jnp.int32),
                pltpu.VMEM(bags_t.shape, jnp.int32),
                pltpu.VMEM(hot_rows.shape, jnp.int32),
                pltpu.SMEM(hot_rows.shape, jnp.int32),
                pltpu.VMEM(ids_t.shape, jnp.int32),
                pltpu.VMEM((peers, 1, lanes), jnp.int32),
                pltpu.SMEM((peers, 1, lanes), jnp.int32),
                pltpu.VMEM((peers, tcount * cap, width), jnp.float32),
                pltpu.VMEM((peers, tcount * cap, width), jnp.float32),
                pltpu.VMEM((tcount * hot, width), jnp.float32),
                pltpu.VMEM((tcount * hot, width), jnp.float32),
                pltpu.VMEM((ny // 2, chunk, width), jnp.float32),
                pltpu.VMEM((levels, chunk, width), jnp.float32),
                pltpu.VMEM((levels, chunk, width), jnp.float32),
                pltpu.VMEM((tcount * hot, width), jnp.float32),
                pltpu.VMEM((tcount, batch, peers * cap), jnp.bfloat16),
                pltpu.VMEM((tcount, batch, hot), jnp.bfloat16),
                pltpu.SemaphoreType.DMA((tcount, CHUNKS)),
                pltpu.SemaphoreType.DMA((4,)),
                pltpu.SemaphoreType.DMA,
                pltpu.SemaphoreType.DMA,
                pltpu.SemaphoreType.DMA((peers,)),
                pltpu.SemaphoreType.DMA,
                pltpu.SemaphoreType.DMA,
                pltpu.SemaphoreType.DMA((nx,)),
                pltpu.SemaphoreType.DMA((tcount,)),
                pltpu.SemaphoreType.DMA((tcount,)),
                pltpu.SemaphoreType.DMA,
                pltpu.SemaphoreType.DMA,
                pltpu.SemaphoreType.DMA((levels,)),
                pltpu.SemaphoreType.DMA((levels,)),
                pltpu.SemaphoreType.DMA,
                pltpu.SemaphoreType.DMA((ny // 2,)),
                pltpu.SemaphoreType.DMA,
                pltpu.SemaphoreType.DMA,
            ] + [pltpu.VMEM((rows_dev + PAD, width), jnp.float32)] * tcount,
            compiler_params=pltpu.CompilerParams(
                collective_id=0, has_side_effects=True,
                vmem_limit_bytes=VMEM_BYTES - 4 * batch * tcount * width),
        )(tables, rows_t, bags_t, hot_rows, ids_t)
        return out.reshape(batch, tcount, width)

    return jax.shard_map(
        body,
        mesh=mesh,
        in_specs=(
            P(None, ("gx", "gy"), None),
            P(("gx", "gy"), None, None, None),
            P(("gx", "gy"), None, None, None),
            P(),
            P(("gx", "gy"), None, None),
        ),
        out_specs=P(("gx", "gy"), None, None),
        check_vma=False,
    )
```

```python
import functools

import jax
import jax.numpy as jnp
from jax import lax
from jax.experimental import pallas as pl
from jax.experimental.pallas import tpu as pltpu
from jax.sharding import PartitionSpec as P

MESH = pl.DeviceIdType.MESH
CHUNKS = 4
PAD = 8
COLUMN = 2
VMEM_BYTES = 67043328


def split2(x):
    hi = x.astype(jnp.bfloat16)
    return hi, (x - hi.astype(jnp.float32)).astype(jnp.bfloat16)


def pool(weights, values):
    hi, lo = split2(values)
    return jnp.dot(weights, hi, preferred_element_type=jnp.float32) + jnp.dot(
        weights, lo, preferred_element_type=jnp.float32
    )


def plane_order(nx, u):
    rest = [q for q in range(nx) if q not in (u, u + 1)]
    return [u + 1, u] + sorted(rest, key=lambda q: (abs(q - u), q < u))


def kernel(nx, ny, tables_ref, rows_hbm, bags_hbm, hot_rows_hbm, hot_ids_hbm, out_ref,
           rows_ref, bags_ref, hot_rows_ref, hot_at, hot_ids_ref,
           idx_out, idx_s, stage, recv, hot_stage, pair_in, hot_in, hot_sum, hot_z, hot_tab,
           onehot, counts, load_sem, sent, idx_recv, cold_recv,
           pair_recv, hot_recv, z_recv, gat_recv, fwd_recv, *tabs):
    peers = nx * ny
    half, chips = nx // 2, ny // 2
    tcount, rows_dev, width = tables_ref.shape
    cap = rows_ref.shape[1]
    hot = hot_rows_ref.shape[1]
    chunk = hot // chips
    batch = out_ref.shape[0] // tcount
    levels = nx.bit_length() - 1
    gx, gy = lax.axis_index("gx"), lax.axis_index("gy")
    me = gx * ny + gy
    chip, core = gy // 2, lax.rem(gy, 2)
    partner = gy + 1 - 2 * core
    hub = core == 1
    low = gx < half
    u = jnp.where(low, gx, nx - 1 - gx)

    orders = [plane_order(nx, k) for k in range(half)]
    px_of = []
    for m in range(nx):
        q = jnp.int32(orders[0][m])
        for k in range(1, half):
            q = jnp.where(u == k, orders[k][m], q)
        px_of.append(jnp.where(low, q, nx - 1 - q))

    def flip(v, n, j):
        y, b = 0, 1
        while b < n:
            y += lax.rem(v // b + j // b, 2) * b
            b *= 2
        return y

    py_of = [flip(gy, ny, j) for j in range(ny)]

    def span_of(m, first, last):
        return range(max(first, 1) if m == 1 else first, last)

    def remote(src, dst, recv_sem, px, py):
        return pltpu.make_async_remote_copy(
            src_ref=src, dst_ref=dst, send_sem=sent, recv_sem=recv_sem,
            device_id=(px, py), device_id_type=MESH)

    def arrived(ref, sem):
        pltpu.make_async_copy(ref, ref, sem).wait()

    small = [pltpu.make_async_copy(src, dst, load_sem.at[n]) for n, src, dst in (
        (0, rows_hbm, rows_ref), (1, hot_rows_hbm, hot_rows_ref),
        (2, bags_hbm, bags_ref), (3, hot_ids_hbm, hot_ids_ref))]
    small[0].start()
    small[1].start()

    barrier = pltpu.get_barrier_semaphore()
    for m in reversed(range(nx)):
        for j in span_of(m, 0, ny):
            pl.semaphore_signal(
                barrier, inc=1, device_id=(px_of[m], py_of[j]), device_id_type=MESH)

    piece = rows_dev // CHUNKS
    for t in range(tcount):
        for c in range(CHUNKS):
            part = pl.ds(c * piece, piece)
            pltpu.make_async_copy(
                tables_ref.at[t, part], tabs[t].at[part], load_sem.at[4 + t]).start()
    small[2].start()
    small[3].start()
    for t in range(tcount):
        tabs[t][rows_dev:rows_dev + PAD, :] = jnp.zeros((PAD, width), jnp.float32)

    small[1].wait()
    local = hot_rows_ref[...] - me * rows_dev
    hot_rows_ref[...] = jnp.where(
        jnp.logical_and(local >= 0, local < rows_dev), local, rows_dev)
    small[0].wait()
    where_hot = pltpu.make_async_copy(hot_rows_ref, hot_at, load_sem.at[1])
    where_hot.start()
    lines = rows_ref[...].reshape(tcount * cap, peers).T
    for p in range(peers):
        idx_out[p, :, 0:tcount * cap] = lines[p:p + 1, :]
    own_idx = pltpu.make_async_copy(idx_out.at[me], idx_s.at[me], load_sem.at[0])
    own_idx.start()

    group = min(hot, 32)

    def pick_hot(t):
        whole = pl.ds(0, rows_dev)
        arrived(tabs[t].at[whole], load_sem.at[4 + t])

        def step(g, carry):
            for j in range(group):
                hot_stage[pl.ds(t * hot + g * group + j, 1), :] = tabs[t][
                    pl.ds(hot_at[t, g * group + j], 1), :]
            return carry
        lax.fori_loop(0, hot // group, step, 0)

    def table_rows(t):
        return pl.ds(t * hot, hot)

    def pair_send(t):
        remote(hot_stage.at[table_rows(t)], pair_in.at[table_rows(t)], pair_recv.at[t],
               gx, partner).start()

    where_hot.wait()
    pick_hot(0)
    pl.semaphore_wait(barrier, peers - 1)
    for m in range(nx):
        for j in span_of(m, 0, ny):
            remote(idx_out.at[px_of[m] * ny + py_of[j]], idx_s.at[me],
                   idx_recv.at[2 * gx + (j >= COLUMN)], px_of[m], py_of[j]).start()

    @pl.when(jnp.logical_not(hub))
    def _():
        pair_send(0)

    for t in range(1, tcount):
        pick_hot(t)

    def pick(p):
        for t in range(tcount):
            for c in range(cap):
                k = t * cap + c
                stage[p, k:k + 1, :] = tabs[t][pl.ds(idx_s[p, 0, k], 1), :]

    def asked(m, far):
        count = ny - COLUMN if far else len(span_of(m, 0, COLUMN))
        arrived(idx_s.at[pl.ds(0, count)], idx_recv.at[2 * px_of[m] + far])

    def take(m, first, last):
        def step(j, carry):
            pick(px_of[m] * ny + flip(gy, ny, j))
            return carry
        span = span_of(m, first, last)
        lax.fori_loop(span.start, span.stop, step, 0)

    def send(m, first, last):
        for j in span_of(m, first, last):
            remote(stage.at[px_of[m] * ny + py_of[j]], recv.at[me], cold_recv.at[gx],
                   px_of[m], py_of[j]).start()

    def rows_of(t, k):
        return pl.ds(pl.multiple_of(t * hot + k * chunk, chunk), chunk)

    def pair_sum(t):
        rows = table_rows(t)
        arrived(pair_in.at[rows], pair_recv.at[t])
        pair_in[rows, :] = pair_in[rows, :] + hot_stage[rows, :]

    def hot_sends(t):
        for k in range(1, chips):
            to = flip(chip, chips, k)
            remote(pair_in.at[rows_of(t, to)], hot_in.at[t, chip], hot_recv.at[t],
                   gx, 2 * to + core).start()
        hot_in[t, chip] = pair_in[rows_of(t, chip), :]

    def hot_reduce(t):
        others = pl.ds(0, chips - 1)
        arrived(hot_in.at[t, others], hot_recv.at[t])
        hot_sum[t, 0] = jnp.sum(hot_in[t], axis=0)

    def z_send(t, k):
        b = 1 << k
        to = gx + b - 2 * b * lax.rem(gx // b, 2)
        remote(hot_sum.at[t, k], hot_z.at[t, k], z_recv.at[t * levels + k], to, gy).start()

    def z_sum(t, k):
        arrived(hot_z.at[t, k], z_recv.at[t * levels + k])
        total = hot_sum[t, k] + hot_z[t, k]
        if k + 1 < levels:
            hot_sum[t, k + 1] = total
        else:
            hot_tab[rows_of(t, chip), :] = total

    def gat_sends(t):
        mine = hot_tab.at[rows_of(t, chip)]
        for k in range(1, chips):
            remote(mine, mine, gat_recv.at[t], gx, 2 * flip(chip, chips, k) + core).start()
        remote(mine, mine, fwd_recv, gx, partner).start()

    def forward(t):
        apart = pl.ds(0, (chips - 1) * chunk)
        arrived(hot_tab.at[apart], gat_recv.at[t])
        for k in range(1, chips):
            got = hot_tab.at[rows_of(t, flip(chip, chips, k))]
            remote(got, got, fwd_recv, gx, partner).start()

    slots = peers * cap
    owner = lax.broadcasted_iota(jnp.int32, (peers, slots), 1) // cap
    spread = (owner == lax.broadcasted_iota(jnp.int32, (peers, slots), 0)).astype(jnp.float32)
    place = lax.rem(lax.broadcasted_iota(jnp.int32, (cap, slots), 1), cap)
    mask = place == lax.broadcasted_iota(jnp.int32, (cap, slots), 0)
    samples = lax.broadcasted_iota(jnp.int32, (batch, slots), 0).astype(jnp.float32)

    def cold_weights(t):
        wide = jnp.dot(bags_ref[t].astype(jnp.float32), spread,
                       precision=lax.Precision.HIGHEST, preferred_element_type=jnp.float32)
        flat = jnp.sum(jnp.where(mask, wide, 0.0), axis=0, keepdims=True)
        onehot[t] = (flat == samples).astype(jnp.bfloat16)

    entry = lax.broadcasted_iota(jnp.int32, (hot, batch), 0)

    def hot_counts(t):
        total = jnp.zeros((hot, batch), jnp.float32)
        for k in range(hot_ids_ref.shape[1]):
            total += (hot_ids_ref[t, k:k + 1, :] == entry).astype(jnp.float32)
        counts[t] = total.T.astype(jnp.bfloat16)

    tables = range(tcount)
    sums = [jnp.zeros((batch, width), jnp.float32) for _ in tables]

    def pool_plane(m):
        arrived(recv.at[pl.ds(0, len(span_of(m, 0, ny)))], cold_recv.at[px_of[m]])
        at = pl.ds(pl.multiple_of(px_of[m] * ny, ny), ny)
        cols = pl.ds(pl.multiple_of(px_of[m] * ny * cap, ny * cap), ny * cap)
        for t in tables:
            values = recv[at, t * cap:(t + 1) * cap, :].reshape(ny * cap, width)
            sums[t] = sums[t] + pool(onehot[t, :, cols], values)

    def pool_hot():
        for t in tables:
            sums[t] = sums[t] + pool(counts[t], hot_tab[t * hot:(t + 1) * hot, :])

    @pl.when(hub)
    def _():
        for m in (0, *range(3, nx)):
            asked(m, 0)
            take(m, 0, COLUMN)
            send(m, 0, COLUMN)
        for t in tables:
            pair_sum(t)
        asked(1, 0)
        take(1, 0, COLUMN)
        for t in tables:
            hot_sends(t)
        asked(2, 0)
        take(2, 0, COLUMN)
        send(2, 0, COLUMN)
        for m in (0, *range(3, nx)):
            asked(m, 1)
            take(m, COLUMN, ny)
        asked(1, 1)
        take(1, COLUMN, ny)
        hot_reduce(0)
        asked(2, 1)
        take(2, COLUMN, ny)
        own_idx.wait()
        pick(me)
        z_send(0, 0)
        for t in range(1, tcount):
            hot_reduce(t)
        recv[me] = stage[me]
        send(1, 0, ny)
        for t in range(1, tcount):
            z_send(t, 0)
        small[2].wait()
        small[3].wait()
        cold_weights(0)
        for k in range(1, levels):
            for t in tables:
                z_sum(t, k - 1)
                hot_counts(t) if k == 1 else None
                z_send(t, k)
        for a in range(COLUMN, ny, 2):
            for m in (*range(3, nx), 0, 2):
                send(m, a, a + 2)
        for t in range(1, tcount):
            cold_weights(t)
        for t in tables:
            z_sum(t, levels - 1)
        gat_sends(0)
        for t in range(1, tcount):
            gat_sends(t)
        for t in tables:
            forward(t)

    @pl.when(jnp.logical_not(hub))
    def _():
        for t in range(1, tcount):
            pair_send(t)
        for m in (0, *range(3, nx), 2):
            asked(m, 0)
            take(m, 0, COLUMN)
            send(m, 0, COLUMN)
        for m in (0, *range(3, nx), 2):
            asked(m, 1)
            take(m, COLUMN, ny)
            send(m, COLUMN, ny)
        asked(1, 0)
        asked(1, 1)
        take(1, 0, ny)
        own_idx.wait()
        pick(me)
        send(1, 0, ny)
        recv[me] = stage[me]
        small[2].wait()
        small[3].wait()
        for t in tables:
            hot_counts(t)
            cold_weights(t)

    pool_plane(1)
    pool_plane(0)

    @pl.when(jnp.logical_not(hub))
    def _():
        arrived(hot_tab, fwd_recv)

    pool_hot()
    for m in range(2, nx):
        pool_plane(m)
    for t in tables:
        out_ref[t::tcount, :] = sums[t]

    lines_sent = (peers - 1) * (idx_out.shape[2] // width + tcount * cap)
    hub_sent = tcount * chunk * (2 * (chips - 1) + levels + chips)

    @pl.when(hub)
    def _():
        arrived(tabs[0].at[pl.ds(0, lines_sent + hub_sent)], sent)

    @pl.when(jnp.logical_not(hub))
    def _():
        arrived(tabs[0].at[pl.ds(0, lines_sent + tcount * hot)], sent)


def solution(mesh):
    nx, ny = mesh.shape["gx"], mesh.shape["gy"]
    peers = nx * ny

    def body(tables, cold_rows, cold_bags, hot_rows, hot_ids):
        tcount, rows_dev, width = tables.shape
        cap = cold_rows.shape[3]
        batch = hot_ids.shape[0]
        hot = hot_rows.shape[1]
        chips = ny // 2
        chunk = hot // chips
        levels = nx.bit_length() - 1
        lanes = -(-tcount * cap // width) * width
        assert nx == 1 << levels and ny & (ny - 1) == 0 and min(nx, ny) > 1
        assert chunk * chips == hot and chunk % 8 == 0 and ny * cap % 128 == 0
        assert rows_dev % CHUNKS == 0 and hot & (hot - 1) == 0
        rows_t = jnp.transpose(cold_rows[0], (0, 2, 1))
        bags_t = jnp.transpose(cold_bags[0], (0, 2, 1))
        ids_t = jnp.transpose(hot_ids, (1, 2, 0))
        hbm = pl.BlockSpec(memory_space=pltpu.HBM)
        f32, sem = jnp.float32, pltpu.SemaphoreType.DMA
        out = pl.pallas_call(
            functools.partial(kernel, nx, ny),
            out_shape=pltpu.VMEM((batch * tcount, width), f32),
            in_specs=[hbm] * 5,
            out_specs=pl.BlockSpec(memory_space=pltpu.VMEM),
            scratch_shapes=[
                pltpu.VMEM(rows_t.shape, jnp.int32),
                pltpu.VMEM(bags_t.shape, jnp.int32),
                pltpu.VMEM(hot_rows.shape, jnp.int32),
                pltpu.SMEM(hot_rows.shape, jnp.int32),
                pltpu.VMEM(ids_t.shape, jnp.int32),
                pltpu.VMEM((peers, 1, lanes), jnp.int32),
                pltpu.SMEM((peers, 1, lanes), jnp.int32),
                pltpu.VMEM((peers, tcount * cap, width), f32),
                pltpu.VMEM((peers, tcount * cap, width), f32),
                pltpu.VMEM((tcount * hot, width), f32),
                pltpu.VMEM((tcount * hot, width), f32),
                pltpu.VMEM((tcount, chips, chunk, width), f32),
                pltpu.VMEM((tcount, levels, chunk, width), f32),
                pltpu.VMEM((tcount, levels, chunk, width), f32),
                pltpu.VMEM((tcount * hot, width), f32),
                pltpu.VMEM((tcount, batch, peers * cap), jnp.bfloat16),
                pltpu.VMEM((tcount, batch, hot), jnp.bfloat16),
                sem((4 + tcount,)),
                sem,
                sem((2 * nx,)),
                sem((nx,)),
                sem((tcount,)),
                sem((tcount,)),
                sem((tcount * levels,)),
                sem((tcount,)),
                sem,
            ] + [pltpu.VMEM((rows_dev + PAD, width), f32)] * tcount,
            compiler_params=pltpu.CompilerParams(
                collective_id=0, has_side_effects=True,
                vmem_limit_bytes=VMEM_BYTES - 4 * batch * tcount * width),
        )(tables, rows_t, bags_t, hot_rows, ids_t)
        return out.reshape(batch, tcount, width)

    return jax.shard_map(
        body,
        mesh=mesh,
        in_specs=(
            P(None, ("gx", "gy"), None),
            P(("gx", "gy"), None, None, None),
            P(("gx", "gy"), None, None, None),
            P(),
            P(("gx", "gy"), None, None),
        ),
        out_specs=P(("gx", "gy"), None, None),
        check_vma=False,
    )
```

```python
import functools

import jax
import jax.numpy as jnp
from jax import lax
from jax.experimental import pallas as pl
from jax.experimental.pallas import tpu as pltpu
from jax.sharding import PartitionSpec as P

MESH = pl.DeviceIdType.MESH
CHUNKS = 4
PAD = 8
COLUMN = 2
VMEM_BYTES = 67043328


def split2(x):
    hi = x.astype(jnp.bfloat16)
    return hi, (x - hi.astype(jnp.float32)).astype(jnp.bfloat16)


def pool(weights, values):
    hi, lo = split2(values)
    return jnp.dot(weights, hi, preferred_element_type=jnp.float32) + jnp.dot(
        weights, lo, preferred_element_type=jnp.float32
    )


def plane_order(nx, u):
    half = nx // 2
    near = sorted((q for q in range(half) if q != u), key=lambda q: abs(q - u))
    return [half, u] + near + list(range(half + 1, nx))


def kernel(nx, ny, tables_ref, rows_hbm, bags_hbm, hot_rows_hbm, hot_ids_hbm, out_ref,
           rows_ref, bags_ref, hot_rows_ref, hot_at, hot_ids_ref,
           idx_out, idx_s, stage, recv, hot_stage, pair_in, hot_in, hot_sum, hot_z, hot_tab,
           onehot, counts, load_sem, sent, idx_recv, cold_recv,
           pair_recv, hot_recv, z_recv, gat_recv, fwd_recv, *tabs):
    peers = nx * ny
    half, chips = nx // 2, ny // 2
    tcount, rows_dev, width = tables_ref.shape
    cap = rows_ref.shape[1]
    hot = hot_rows_ref.shape[1]
    chunk = hot // chips
    batch = out_ref.shape[0] // tcount
    levels = nx.bit_length() - 1
    gx, gy = lax.axis_index("gx"), lax.axis_index("gy")
    me = gx * ny + gy
    chip, core = gy // 2, lax.rem(gy, 2)
    partner = gy + 1 - 2 * core
    hub = core == 1
    low = gx < half
    u = jnp.where(low, gx, nx - 1 - gx)

    orders = [plane_order(nx, k) for k in range(half)]
    px_of = []
    for m in range(nx):
        q = jnp.int32(orders[0][m])
        for k in range(1, half):
            q = jnp.where(u == k, orders[k][m], q)
        px_of.append(jnp.where(low, q, nx - 1 - q))

    def flip(v, n, j):
        y, b = 0, 1
        while b < n:
            y += lax.rem(v // b + j // b, 2) * b
            b *= 2
        return y

    py_of = [flip(gy, ny, j) for j in range(ny)]

    def span_of(m, first, last):
        return range(max(first, 1) if m == 1 else first, min(last, ny))

    def remote(src, dst, recv_sem, px, py):
        return pltpu.make_async_remote_copy(
            src_ref=src, dst_ref=dst, send_sem=sent, recv_sem=recv_sem,
            device_id=(px, py), device_id_type=MESH)

    def arrived(ref, sem):
        pltpu.make_async_copy(ref, ref, sem).wait()

    small = [pltpu.make_async_copy(src, dst, load_sem.at[n]) for n, src, dst in (
        (0, rows_hbm, rows_ref), (1, hot_rows_hbm, hot_rows_ref),
        (2, bags_hbm, bags_ref), (3, hot_ids_hbm, hot_ids_ref))]
    small[0].start()
    small[1].start()

    barrier = pltpu.get_barrier_semaphore()
    for m in reversed(range(nx)):
        for j in span_of(m, 0, ny):
            pl.semaphore_signal(
                barrier, inc=1, device_id=(px_of[m], py_of[j]), device_id_type=MESH)

    piece = rows_dev // CHUNKS
    for t in range(tcount):
        for c in range(CHUNKS):
            part = pl.ds(c * piece, piece)
            pltpu.make_async_copy(
                tables_ref.at[t, part], tabs[t].at[part], load_sem.at[4 + t]).start()
    small[2].start()
    small[3].start()
    for t in range(tcount):
        tabs[t][rows_dev:rows_dev + PAD, :] = jnp.zeros((PAD, width), jnp.float32)

    small[1].wait()
    local = hot_rows_ref[...] - me * rows_dev
    hot_rows_ref[...] = jnp.where(
        jnp.logical_and(local >= 0, local < rows_dev), local, rows_dev)
    small[0].wait()
    where_hot = pltpu.make_async_copy(hot_rows_ref, hot_at, load_sem.at[1])
    where_hot.start()
    lines = rows_ref[...].reshape(tcount * cap, peers).T
    for p in range(peers):
        idx_out[p, :, 0:tcount * cap] = lines[p:p + 1, :]
    own_idx = pltpu.make_async_copy(idx_out.at[me], idx_s.at[me], load_sem.at[0])
    own_idx.start()

    group = min(hot, 32)

    def pick_hot(t):
        whole = pl.ds(0, rows_dev)
        arrived(tabs[t].at[whole], load_sem.at[4 + t])

        def step(g, carry):
            for j in range(group):
                hot_stage[pl.ds(t * hot + g * group + j, 1), :] = tabs[t][
                    pl.ds(hot_at[t, g * group + j], 1), :]
            return carry
        lax.fori_loop(0, hot // group, step, 0)

    def table_rows(t):
        return pl.ds(t * hot, hot)

    def pair_send(t):
        remote(hot_stage.at[table_rows(t)], pair_in.at[table_rows(t)], pair_recv.at[t],
               gx, partner).start()

    where_hot.wait()
    pick_hot(0)
    pl.semaphore_wait(barrier, peers - 1)
    for m in range(nx):
        for j in span_of(m, 0, ny):
            remote(idx_out.at[px_of[m] * ny + py_of[j]], idx_s.at[me],
                   idx_recv.at[2 * gx + (j >= COLUMN)], px_of[m], py_of[j]).start()

    @pl.when(jnp.logical_not(hub))
    def _():
        pair_send(0)

    for t in range(1, tcount):
        pick_hot(t)

    def pick(p):
        for t in range(tcount):
            for c in range(cap):
                k = t * cap + c
                stage[p, k:k + 1, :] = tabs[t][pl.ds(idx_s[p, 0, k], 1), :]

    def asked(m, far):
        count = ny - COLUMN if far else len(span_of(m, 0, COLUMN))
        arrived(idx_s.at[pl.ds(0, count)], idx_recv.at[2 * px_of[m] + far])

    def take(m, first, last):
        def step(j, carry):
            pick(px_of[m] * ny + flip(gy, ny, j))
            return carry
        span = span_of(m, first, last)
        lax.fori_loop(span.start, span.stop, step, 0)

    def send(m, first, last):
        for j in span_of(m, first, last):
            remote(stage.at[px_of[m] * ny + py_of[j]], recv.at[me], cold_recv.at[gx],
                   px_of[m], py_of[j]).start()

    def rows_of(t, k):
        return pl.ds(pl.multiple_of(t * hot + k * chunk, chunk), chunk)

    def pair_sum(t):
        rows = table_rows(t)
        arrived(pair_in.at[rows], pair_recv.at[t])
        pair_in[rows, :] = pair_in[rows, :] + hot_stage[rows, :]

    def hot_sends(t):
        for k in range(1, chips):
            to = flip(chip, chips, k)
            remote(pair_in.at[rows_of(t, to)], hot_in.at[t, chip], hot_recv.at[t],
                   gx, 2 * to + core).start()
        hot_in[t, chip] = pair_in[rows_of(t, chip), :]

    def hot_reduce(t):
        others = pl.ds(0, chips - 1)
        arrived(hot_in.at[t, others], hot_recv.at[t])
        hot_sum[t, 0] = jnp.sum(hot_in[t], axis=0)

    def z_send(t, k):
        b = 1 << k
        to = gx + b - 2 * b * lax.rem(gx // b, 2)
        remote(hot_sum.at[t, k], hot_z.at[t, k], z_recv.at[t * levels + k], to, gy).start()

    def z_sum(t, k):
        arrived(hot_z.at[t, k], z_recv.at[t * levels + k])
        total = hot_sum[t, k] + hot_z[t, k]
        if k + 1 < levels:
            hot_sum[t, k + 1] = total
        else:
            hot_tab[rows_of(t, chip), :] = total

    def gat_sends(t):
        mine = hot_tab.at[rows_of(t, chip)]
        for k in range(1, chips):
            remote(mine, mine, gat_recv.at[t], gx, 2 * flip(chip, chips, k) + core).start()
        remote(mine, mine, fwd_recv, gx, partner).start()

    def forward(t):
        apart = pl.ds(0, (chips - 1) * chunk)
        arrived(hot_tab.at[apart], gat_recv.at[t])
        for k in range(1, chips):
            got = hot_tab.at[rows_of(t, flip(chip, chips, k))]
            remote(got, got, fwd_recv, gx, partner).start()

    slots = peers * cap
    owner = lax.broadcasted_iota(jnp.int32, (peers, slots), 1) // cap
    spread = (owner == lax.broadcasted_iota(jnp.int32, (peers, slots), 0)).astype(jnp.float32)
    place = lax.rem(lax.broadcasted_iota(jnp.int32, (cap, slots), 1), cap)
    mask = place == lax.broadcasted_iota(jnp.int32, (cap, slots), 0)
    samples = lax.broadcasted_iota(jnp.int32, (batch, slots), 0).astype(jnp.float32)

    def cold_weights(t):
        wide = jnp.dot(bags_ref[t].astype(jnp.float32), spread,
                       precision=lax.Precision.HIGHEST, preferred_element_type=jnp.float32)
        flat = jnp.sum(jnp.where(mask, wide, 0.0), axis=0, keepdims=True)
        onehot[t] = (flat == samples).astype(jnp.bfloat16)

    entry = lax.broadcasted_iota(jnp.int32, (hot, batch), 0)

    def hot_counts(t):
        total = jnp.zeros((hot, batch), jnp.float32)
        for k in range(hot_ids_ref.shape[1]):
            total += (hot_ids_ref[t, k:k + 1, :] == entry).astype(jnp.float32)
        counts[t] = total.T.astype(jnp.bfloat16)

    tables = range(tcount)
    sums = [jnp.zeros((batch, width), jnp.float32) for _ in tables]

    def pool_plane(m):
        arrived(recv.at[pl.ds(0, len(span_of(m, 0, ny)))], cold_recv.at[px_of[m]])
        at = pl.ds(pl.multiple_of(px_of[m] * ny, ny), ny)
        cols = pl.ds(pl.multiple_of(px_of[m] * ny * cap, ny * cap), ny * cap)
        for t in tables:
            values = recv[at, t * cap:(t + 1) * cap, :].reshape(ny * cap, width)
            sums[t] = sums[t] + pool(onehot[t, :, cols], values)

    def pool_hot():
        for t in tables:
            sums[t] = sums[t] + pool(counts[t], hot_tab[t * hot:(t + 1) * hot, :])

    @pl.when(hub)
    def _():
        pair_sum(0)
        small[2].wait()
        small[3].wait()
        hot_counts(0)
        hot_sends(0)
        for m in (0, *range(3, nx)):
            asked(m, 0)
            take(m, 0, COLUMN)
            send(m, 0, COLUMN)
        for t in range(1, tcount):
            pair_sum(t)
        asked(1, 0)
        take(1, 0, COLUMN)
        for t in range(1, tcount):
            hot_sends(t)
        asked(2, 0)
        take(2, 0, COLUMN)
        send(2, 0, COLUMN)
        for m in (0, *range(3, nx)):
            asked(m, 1)
            take(m, COLUMN, ny)
        asked(1, 1)
        take(1, COLUMN, ny)
        hot_reduce(0)
        asked(2, 1)
        take(2, COLUMN, ny)
        z_send(0, 0)
        for t in range(1, tcount):
            hot_reduce(t)
        own_idx.wait()
        pick(me)
        recv[me] = stage[me]
        for t in range(1, tcount):
            z_send(t, 0)
        for k in range(1, levels):
            for t in tables:
                z_sum(t, k - 1)
                if k == 1 and t == 1:
                    send(1, 0, ny)
                if k == 1 and t == 0:
                    for other in range(1, tcount):
                        hot_counts(other)
                z_send(t, k)
        for a in reversed(range(COLUMN, ny, 2)):
            for m in (*range(3, nx), 0):
                send(m, a, a + 2)
        for a in reversed(range(COLUMN, ny, 2)):
            send(2, a, a + 2)
        for t in tables:
            z_sum(t, levels - 1)
            cold_weights(t)
            gat_sends(t)
        for t in tables:
            forward(t)

    @pl.when(jnp.logical_not(hub))
    def _():
        for t in range(1, tcount):
            pair_send(t)
        for m in (0, *range(3, nx)):
            asked(m, 0)
            take(m, 0, COLUMN)
            send(m, 0, COLUMN)
        for a in reversed(range(COLUMN, ny, 2)):
            for m in (0, *range(3, nx)):
                asked(m, 1) if a + 2 >= ny else None
                take(m, a, a + 2)
                send(m, a, a + 2)
        asked(2, 0)
        asked(2, 1)
        take(2, 0, ny)
        send(2, 0, ny)
        asked(1, 0)
        asked(1, 1)
        take(1, 0, ny)
        own_idx.wait()
        pick(me)
        send(1, 0, ny)
        recv[me] = stage[me]
        small[2].wait()
        small[3].wait()
        for t in tables:
            hot_counts(t)
            cold_weights(t)

    pool_plane(1)
    pool_plane(0)

    @pl.when(jnp.logical_not(hub))
    def _():
        arrived(hot_tab, fwd_recv)

    pool_hot()
    for m in range(2, nx):
        pool_plane(m)
    for t in tables:
        out_ref[t::tcount, :] = sums[t]

    lines_sent = (peers - 1) * (idx_out.shape[2] // width + tcount * cap)
    hub_sent = tcount * chunk * (2 * (chips - 1) + levels + chips)

    @pl.when(hub)
    def _():
        arrived(tabs[0].at[pl.ds(0, lines_sent + hub_sent)], sent)

    @pl.when(jnp.logical_not(hub))
    def _():
        arrived(tabs[0].at[pl.ds(0, lines_sent + tcount * hot)], sent)


def solution(mesh):
    nx, ny = mesh.shape["gx"], mesh.shape["gy"]
    peers = nx * ny

    def body(tables, cold_rows, cold_bags, hot_rows, hot_ids):
        tcount, rows_dev, width = tables.shape
        cap = cold_rows.shape[3]
        batch = hot_ids.shape[0]
        hot = hot_rows.shape[1]
        chips = ny // 2
        chunk = hot // chips
        levels = nx.bit_length() - 1
        lanes = -(-tcount * cap // width) * width
        assert nx == 1 << levels and ny & (ny - 1) == 0 and min(nx, ny) > 1
        assert chunk * chips == hot and chunk % 8 == 0 and ny * cap % 128 == 0
        assert rows_dev % CHUNKS == 0 and hot & (hot - 1) == 0
        rows_t = jnp.transpose(cold_rows[0], (0, 2, 1))
        bags_t = jnp.transpose(cold_bags[0], (0, 2, 1))
        ids_t = jnp.transpose(hot_ids, (1, 2, 0))
        hbm = pl.BlockSpec(memory_space=pltpu.HBM)
        f32, sem = jnp.float32, pltpu.SemaphoreType.DMA
        out = pl.pallas_call(
            functools.partial(kernel, nx, ny),
            out_shape=pltpu.VMEM((batch * tcount, width), f32),
            in_specs=[hbm] * 5,
            out_specs=pl.BlockSpec(memory_space=pltpu.VMEM),
            scratch_shapes=[
                pltpu.VMEM(rows_t.shape, jnp.int32),
                pltpu.VMEM(bags_t.shape, jnp.int32),
                pltpu.VMEM(hot_rows.shape, jnp.int32),
                pltpu.SMEM(hot_rows.shape, jnp.int32),
                pltpu.VMEM(ids_t.shape, jnp.int32),
                pltpu.VMEM((peers, 1, lanes), jnp.int32),
                pltpu.SMEM((peers, 1, lanes), jnp.int32),
                pltpu.VMEM((peers, tcount * cap, width), f32),
                pltpu.VMEM((peers, tcount * cap, width), f32),
                pltpu.VMEM((tcount * hot, width), f32),
                pltpu.VMEM((tcount * hot, width), f32),
                pltpu.VMEM((tcount, chips, chunk, width), f32),
                pltpu.VMEM((tcount, levels, chunk, width), f32),
                pltpu.VMEM((tcount, levels, chunk, width), f32),
                pltpu.VMEM((tcount * hot, width), f32),
                pltpu.VMEM((tcount, batch, peers * cap), jnp.bfloat16),
                pltpu.VMEM((tcount, batch, hot), jnp.bfloat16),
                sem((4 + tcount,)),
                sem,
                sem((2 * nx,)),
                sem((nx,)),
                sem((tcount,)),
                sem((tcount,)),
                sem((tcount * levels,)),
                sem((tcount,)),
                sem,
            ] + [pltpu.VMEM((rows_dev + PAD, width), f32)] * tcount,
            compiler_params=pltpu.CompilerParams(
                collective_id=0, has_side_effects=True,
                vmem_limit_bytes=VMEM_BYTES - 4 * batch * tcount * width),
        )(tables, rows_t, bags_t, hot_rows, ids_t)
        return out.reshape(batch, tcount, width)

    return jax.shard_map(
        body,
        mesh=mesh,
        in_specs=(
            P(None, ("gx", "gy"), None),
            P(("gx", "gy"), None, None, None),
            P(("gx", "gy"), None, None, None),
            P(),
            P(("gx", "gy"), None, None),
        ),
        out_specs=P(("gx", "gy"), None, None),
        check_vma=False,
    )
```

```python
import functools

import jax
import jax.numpy as jnp
from jax import lax
from jax.experimental import pallas as pl
from jax.experimental.pallas import tpu as pltpu
from jax.sharding import PartitionSpec as P

MESH = pl.DeviceIdType.MESH
CHUNKS = 4
PAD = 8
COLUMN = 2
VMEM_BYTES = 67043328


def split2(x):
    hi = x.astype(jnp.bfloat16)
    return hi, (x - hi.astype(jnp.float32)).astype(jnp.bfloat16)


def pool(weights, values):
    hi, lo = split2(values)
    return jnp.dot(weights, hi, preferred_element_type=jnp.float32) + jnp.dot(
        weights, lo, preferred_element_type=jnp.float32
    )


def plane_order(nx, u):
    half = nx // 2
    near = sorted((q for q in range(half) if q != u), key=lambda q: abs(q - u))
    return [half, u] + near + list(range(half + 1, nx))


def kernel(nx, ny, tables_ref, rows_hbm, bags_hbm, hot_rows_hbm, hot_ids_hbm, out_ref,
           rows_ref, bags_ref, hot_rows_ref, hot_at, hot_ids_ref,
           idx_out, idx_s, stage, recv, hot_stage, pair_in, hot_in, hot_sum, hot_z, hot_tab,
           onehot, counts, load_sem, sent, idx_recv, cold_recv,
           pair_recv, hot_recv, z_recv, gat_recv, fwd_recv, *tabs):
    peers = nx * ny
    half, chips = nx // 2, ny // 2
    tcount, rows_dev, width = tables_ref.shape
    cap = rows_ref.shape[1]
    hot = hot_rows_ref.shape[1]
    chunk = hot // chips
    batch = out_ref.shape[0] // tcount
    levels = nx.bit_length() - 1
    gx, gy = lax.axis_index("gx"), lax.axis_index("gy")
    me = gx * ny + gy
    chip, core = gy // 2, lax.rem(gy, 2)
    partner = gy + 1 - 2 * core
    hub = core == 1
    low = gx < half
    u = jnp.where(low, gx, nx - 1 - gx)

    orders = [plane_order(nx, k) for k in range(half)]
    px_of = []
    for m in range(nx):
        q = jnp.int32(orders[0][m])
        for k in range(1, half):
            q = jnp.where(u == k, orders[k][m], q)
        px_of.append(jnp.where(low, q, nx - 1 - q))

    def flip(v, n, j):
        y, b = 0, 1
        while b < n:
            y += lax.rem(v // b + j // b, 2) * b
            b *= 2
        return y

    py_of = [flip(gy, ny, j) for j in range(ny)]

    def span_of(m, first, last):
        return range(max(first, 1) if m == 1 else first, min(last, ny))

    def remote(src, dst, recv_sem, px, py):
        return pltpu.make_async_remote_copy(
            src_ref=src, dst_ref=dst, send_sem=sent, recv_sem=recv_sem,
            device_id=(px, py), device_id_type=MESH)

    def arrived(ref, sem):
        pltpu.make_async_copy(ref, ref, sem).wait()

    small = [pltpu.make_async_copy(src, dst, load_sem.at[n]) for n, src, dst in (
        (0, rows_hbm, rows_ref), (1, hot_rows_hbm, hot_rows_ref),
        (2, bags_hbm, bags_ref), (3, hot_ids_hbm, hot_ids_ref))]
    small[0].start()
    small[1].start()

    barrier = pltpu.get_barrier_semaphore()
    for m in reversed(range(nx)):
        for j in span_of(m, 0, ny):
            pl.semaphore_signal(
                barrier, inc=1, device_id=(px_of[m], py_of[j]), device_id_type=MESH)

    piece = rows_dev // CHUNKS
    for t in range(tcount):
        for c in range(CHUNKS):
            part = pl.ds(c * piece, piece)
            pltpu.make_async_copy(
                tables_ref.at[t, part], tabs[t].at[part], load_sem.at[4 + t]).start()
    small[2].start()
    small[3].start()
    for t in range(tcount):
        tabs[t][rows_dev:rows_dev + PAD, :] = jnp.zeros((PAD, width), jnp.float32)

    small[1].wait()
    local = hot_rows_ref[...] - me * rows_dev
    hot_rows_ref[...] = jnp.where(
        jnp.logical_and(local >= 0, local < rows_dev), local, rows_dev)
    small[0].wait()
    where_hot = pltpu.make_async_copy(hot_rows_ref, hot_at, load_sem.at[1])
    where_hot.start()
    lines = rows_ref[...].reshape(tcount * cap, peers).T
    for p in range(peers):
        idx_out[p, :, 0:tcount * cap] = lines[p:p + 1, :]
    own_idx = pltpu.make_async_copy(idx_out.at[me], idx_s.at[me], load_sem.at[0])
    own_idx.start()

    group = min(hot, 32)

    def pick_hot(t):
        whole = pl.ds(0, rows_dev)
        arrived(tabs[t].at[whole], load_sem.at[4 + t])

        def step(g, carry):
            for j in range(group):
                hot_stage[pl.ds(t * hot + g * group + j, 1), :] = tabs[t][
                    pl.ds(hot_at[t, g * group + j], 1), :]
            return carry
        lax.fori_loop(0, hot // group, step, 0)

    def table_rows(t):
        return pl.ds(t * hot, hot)

    def pair_send(t):
        remote(hot_stage.at[table_rows(t)], pair_in.at[table_rows(t)], pair_recv.at[t],
               gx, partner).start()

    where_hot.wait()
    pick_hot(0)
    pl.semaphore_wait(barrier, peers - 1)
    for m in range(nx):
        for j in span_of(m, 0, ny):
            remote(idx_out.at[px_of[m] * ny + py_of[j]], idx_s.at[me],
                   idx_recv.at[2 * gx + (j >= COLUMN)], px_of[m], py_of[j]).start()

    @pl.when(jnp.logical_not(hub))
    def _():
        pair_send(0)

    for t in range(1, tcount):
        pick_hot(t)

    def pick(p):
        for t in range(tcount):
            for c in range(cap):
                k = t * cap + c
                stage[p, k:k + 1, :] = tabs[t][pl.ds(idx_s[p, 0, k], 1), :]

    def asked(m, far):
        count = ny - COLUMN if far else len(span_of(m, 0, COLUMN))
        arrived(idx_s.at[pl.ds(0, count)], idx_recv.at[2 * px_of[m] + far])

    def take(m, first, last):
        def step(j, carry):
            pick(px_of[m] * ny + flip(gy, ny, j))
            return carry
        span = span_of(m, first, last)
        lax.fori_loop(span.start, span.stop, step, 0)

    def send(m, first, last):
        for j in span_of(m, first, last):
            remote(stage.at[px_of[m] * ny + py_of[j]], recv.at[me], cold_recv.at[gx],
                   px_of[m], py_of[j]).start()

    def rows_of(t, k):
        return pl.ds(pl.multiple_of(t * hot + k * chunk, chunk), chunk)

    def pair_sum(t):
        rows = table_rows(t)
        arrived(pair_in.at[rows], pair_recv.at[t])
        pair_in[rows, :] = pair_in[rows, :] + hot_stage[rows, :]

    def hot_sends(t):
        for k in range(1, chips):
            to = flip(chip, chips, k)
            remote(pair_in.at[rows_of(t, to)], hot_in.at[t, chip], hot_recv.at[t],
                   gx, 2 * to + core).start()
        hot_in[t, chip] = pair_in[rows_of(t, chip), :]

    def hot_reduce(t):
        others = pl.ds(0, chips - 1)
        arrived(hot_in.at[t, others], hot_recv.at[t])
        hot_sum[t, 0] = jnp.sum(hot_in[t], axis=0)

    def z_send(t, k):
        b = 1 << k
        to = gx + b - 2 * b * lax.rem(gx // b, 2)
        remote(hot_sum.at[t, k], hot_z.at[t, k], z_recv.at[t * levels + k], to, gy).start()

    def z_sum(t, k):
        arrived(hot_z.at[t, k], z_recv.at[t * levels + k])
        total = hot_sum[t, k] + hot_z[t, k]
        if k + 1 < levels:
            hot_sum[t, k + 1] = total
        else:
            hot_tab[rows_of(t, chip), :] = total

    def gat_sends(t):
        mine = hot_tab.at[rows_of(t, chip)]
        for k in range(1, chips):
            remote(mine, mine, gat_recv.at[t], gx, 2 * flip(chip, chips, k) + 1 - t % 2).start()
        remote(mine, mine, fwd_recv, gx, partner).start()

    def forward(t):
        apart = pl.ds(0, (chips - 1) * chunk)
        arrived(hot_tab.at[apart], gat_recv.at[t])
        for k in range(1, chips):
            got = hot_tab.at[rows_of(t, flip(chip, chips, k))]
            remote(got, got, fwd_recv, gx, partner).start()

    slots = peers * cap
    owner = lax.broadcasted_iota(jnp.int32, (peers, slots), 1) // cap
    spread = (owner == lax.broadcasted_iota(jnp.int32, (peers, slots), 0)).astype(jnp.float32)
    place = lax.rem(lax.broadcasted_iota(jnp.int32, (cap, slots), 1), cap)
    mask = place == lax.broadcasted_iota(jnp.int32, (cap, slots), 0)
    samples = lax.broadcasted_iota(jnp.int32, (batch, slots), 0).astype(jnp.float32)

    def cold_weights(t):
        wide = jnp.dot(bags_ref[t].astype(jnp.float32), spread,
                       precision=lax.Precision.HIGHEST, preferred_element_type=jnp.float32)
        flat = jnp.sum(jnp.where(mask, wide, 0.0), axis=0, keepdims=True)
        onehot[t] = (flat == samples).astype(jnp.bfloat16)

    entry = lax.broadcasted_iota(jnp.int32, (hot, batch), 0)

    def hot_counts(t):
        total = jnp.zeros((hot, batch), jnp.float32)
        for k in range(hot_ids_ref.shape[1]):
            total += (hot_ids_ref[t, k:k + 1, :] == entry).astype(jnp.float32)
        counts[t] = total.T.astype(jnp.bfloat16)

    tables = range(tcount)
    sums = [jnp.zeros((batch, width), jnp.float32) for _ in tables]

    def pool_plane(m):
        arrived(recv.at[pl.ds(0, len(span_of(m, 0, ny)))], cold_recv.at[px_of[m]])
        at = pl.ds(pl.multiple_of(px_of[m] * ny, ny), ny)
        cols = pl.ds(pl.multiple_of(px_of[m] * ny * cap, ny * cap), ny * cap)
        for t in tables:
            values = recv[at, t * cap:(t + 1) * cap, :].reshape(ny * cap, width)
            sums[t] = sums[t] + pool(onehot[t, :, cols], values)

    def pool_hot():
        for t in tables:
            sums[t] = sums[t] + pool(counts[t], hot_tab[t * hot:(t + 1) * hot, :])

    @pl.when(hub)
    def _():
        pair_sum(0)
        small[2].wait()
        small[3].wait()
        hot_counts(0)
        hot_sends(0)
        for m in (0, *range(3, nx)):
            asked(m, 0)
            take(m, 0, COLUMN)
            send(m, 0, COLUMN)
        for t in range(1, tcount):
            pair_sum(t)
        asked(1, 0)
        take(1, 0, COLUMN)
        for t in range(1, tcount):
            hot_sends(t)
        asked(2, 0)
        take(2, 0, COLUMN)
        send(2, 0, COLUMN)
        for m in (0, *range(3, nx)):
            asked(m, 1)
            take(m, COLUMN, ny)
        asked(1, 1)
        take(1, COLUMN, ny)
        hot_reduce(0)
        asked(2, 1)
        take(2, COLUMN, ny)
        z_send(0, 0)
        for t in range(1, tcount):
            hot_reduce(t)
        own_idx.wait()
        pick(me)
        recv[me] = stage[me]
        for t in range(1, tcount):
            z_send(t, 0)
        for k in range(1, levels):
            for t in tables:
                z_sum(t, k - 1)
                if k == 1 and t == 1:
                    send(1, 0, ny)
                if k == 1 and t == 0:
                    for other in range(1, tcount):
                        hot_counts(other)
                z_send(t, k)
        for a in reversed(range(COLUMN, ny, 2)):
            send(2, a, a + 2)
        for a in reversed(range(COLUMN, ny, 2)):
            for m in (*range(3, nx), 0):
                send(m, a, a + 2)
        for t in tables:
            z_sum(t, levels - 1)
            cold_weights(t)
            gat_sends(t)
        for t in range(0, tcount, 2):
            forward(t)

    @pl.when(jnp.logical_not(hub))
    def _():
        for t in range(1, tcount):
            pair_send(t)
        for m in (0, *range(3, nx)):
            asked(m, 0)
            take(m, 0, COLUMN)
            send(m, 0, COLUMN)
        for a in reversed(range(COLUMN, ny, 2)):
            for m in (0, *range(3, nx)):
                asked(m, 1) if a + 2 >= ny else None
                take(m, a, a + 2)
                send(m, a, a + 2)
        asked(2, 0)
        asked(2, 1)
        take(2, 0, ny)
        send(2, 0, ny)
        asked(1, 0)
        asked(1, 1)
        take(1, 0, ny)
        own_idx.wait()
        pick(me)
        send(1, 0, ny)
        recv[me] = stage[me]
        small[2].wait()
        small[3].wait()
        for t in tables:
            hot_counts(t)
            cold_weights(t)

    pool_plane(1)
    pool_plane(2)

    @pl.when(jnp.logical_not(hub))
    def _():
        for t in range(1, tcount, 2):
            forward(t)

    odds = tcount // 2 * (chips - 1)
    evens = tcount + (tcount - tcount // 2) * (chips - 1)

    @pl.when(hub)
    def _():
        arrived(hot_tab.at[pl.ds(0, odds * chunk)], fwd_recv)

    @pl.when(jnp.logical_not(hub))
    def _():
        arrived(hot_tab.at[pl.ds(0, evens * chunk)], fwd_recv)

    pool_hot()
    for m in (*range(3, nx), 0):
        pool_plane(m)
    for t in tables:
        out_ref[t::tcount, :] = sums[t]

    lines_sent = (peers - 1) * (idx_out.shape[2] // width + tcount * cap)
    odd = tcount // 2
    hub_sent = chunk * (tcount * (2 * (chips - 1) + levels + 1) + (tcount - odd) * (chips - 1))
    spoke_sent = tcount * hot + odd * (chips - 1) * chunk

    @pl.when(hub)
    def _():
        arrived(tabs[0].at[pl.ds(0, lines_sent + hub_sent)], sent)

    @pl.when(jnp.logical_not(hub))
    def _():
        arrived(tabs[0].at[pl.ds(0, lines_sent + spoke_sent)], sent)


def solution(mesh):
    nx, ny = mesh.shape["gx"], mesh.shape["gy"]
    peers = nx * ny

    def body(tables, cold_rows, cold_bags, hot_rows, hot_ids):
        tcount, rows_dev, width = tables.shape
        cap = cold_rows.shape[3]
        batch = hot_ids.shape[0]
        hot = hot_rows.shape[1]
        chips = ny // 2
        chunk = hot // chips
        levels = nx.bit_length() - 1
        lanes = -(-tcount * cap // width) * width
        assert nx == 1 << levels and ny & (ny - 1) == 0 and min(nx, ny) > 1
        assert chunk * chips == hot and chunk % 8 == 0 and ny * cap % 128 == 0
        assert rows_dev % CHUNKS == 0 and hot & (hot - 1) == 0
        rows_t = jnp.transpose(cold_rows[0], (0, 2, 1))
        bags_t = jnp.transpose(cold_bags[0], (0, 2, 1))
        ids_t = jnp.transpose(hot_ids, (1, 2, 0))
        hbm = pl.BlockSpec(memory_space=pltpu.HBM)
        f32, sem = jnp.float32, pltpu.SemaphoreType.DMA
        out = pl.pallas_call(
            functools.partial(kernel, nx, ny),
            out_shape=pltpu.VMEM((batch * tcount, width), f32),
            in_specs=[hbm] * 5,
            out_specs=pl.BlockSpec(memory_space=pltpu.VMEM),
            scratch_shapes=[
                pltpu.VMEM(rows_t.shape, jnp.int32),
                pltpu.VMEM(bags_t.shape, jnp.int32),
                pltpu.VMEM(hot_rows.shape, jnp.int32),
                pltpu.SMEM(hot_rows.shape, jnp.int32),
                pltpu.VMEM(ids_t.shape, jnp.int32),
                pltpu.VMEM((peers, 1, lanes), jnp.int32),
                pltpu.SMEM((peers, 1, lanes), jnp.int32),
                pltpu.VMEM((peers, tcount * cap, width), f32),
                pltpu.VMEM((peers, tcount * cap, width), f32),
                pltpu.VMEM((tcount * hot, width), f32),
                pltpu.VMEM((tcount * hot, width), f32),
                pltpu.VMEM((tcount, chips, chunk, width), f32),
                pltpu.VMEM((tcount, levels, chunk, width), f32),
                pltpu.VMEM((tcount, levels, chunk, width), f32),
                pltpu.VMEM((tcount * hot, width), f32),
                pltpu.VMEM((tcount, batch, peers * cap), jnp.bfloat16),
                pltpu.VMEM((tcount, batch, hot), jnp.bfloat16),
                sem((4 + tcount,)),
                sem,
                sem((2 * nx,)),
                sem((nx,)),
                sem((tcount,)),
                sem((tcount,)),
                sem((tcount * levels,)),
                sem((tcount,)),
                sem,
            ] + [pltpu.VMEM((rows_dev + PAD, width), f32)] * tcount,
            compiler_params=pltpu.CompilerParams(
                collective_id=0, has_side_effects=True,
                vmem_limit_bytes=VMEM_BYTES - 4 * batch * tcount * width),
        )(tables, rows_t, bags_t, hot_rows, ids_t)
        return out.reshape(batch, tcount, width)

    return jax.shard_map(
        body,
        mesh=mesh,
        in_specs=(
            P(None, ("gx", "gy"), None),
            P(("gx", "gy"), None, None, None),
            P(("gx", "gy"), None, None, None),
            P(),
            P(("gx", "gy"), None, None),
        ),
        out_specs=P(("gx", "gy"), None, None),
        check_vma=False,
    )
```

```python
import functools

import jax
import jax.numpy as jnp
from jax import lax
from jax.experimental import pallas as pl
from jax.experimental.pallas import tpu as pltpu
from jax.sharding import PartitionSpec as P

MESH = pl.DeviceIdType.MESH
CHUNKS = 4
PAD = 8
COLUMN = 2
VMEM_BYTES = 67043328


def split2(x):
    hi = x.astype(jnp.bfloat16)
    return hi, (x - hi.astype(jnp.float32)).astype(jnp.bfloat16)


def pool(weights, values):
    hi, lo = split2(values)
    return jnp.dot(weights, hi, preferred_element_type=jnp.float32) + jnp.dot(
        weights, lo, preferred_element_type=jnp.float32
    )


def plane_order(nx, u):
    half = nx // 2
    near = sorted((q for q in range(half) if q != u), key=lambda q: abs(q - u))
    return [half, u] + near + list(range(half + 1, nx))


def kernel(nx, ny, tables_ref, rows_hbm, bags_hbm, hot_rows_hbm, hot_ids_hbm, out_ref,
           rows_ref, bags_ref, hot_rows_ref, hot_at, hot_ids_ref,
           idx_out, idx_s, stage, recv, hot_stage, pair_in, hot_in, hot_sum, hot_z, hot_tab,
           onehot, counts, load_sem, sent, idx_recv, cold_recv,
           pair_recv, hot_recv, z_recv, *tabs):
    peers = nx * ny
    half, chips = nx // 2, ny // 2
    tcount, rows_dev, width = tables_ref.shape
    cap = rows_ref.shape[1]
    hot = hot_rows_ref.shape[1]
    chunk = hot // chips
    batch = out_ref.shape[0] // tcount
    levels = nx.bit_length() - 1
    gx, gy = lax.axis_index("gx"), lax.axis_index("gy")
    me = gx * ny + gy
    chip, core = gy // 2, lax.rem(gy, 2)
    partner = gy + 1 - 2 * core
    hub = core == 1
    low = gx < half
    u = jnp.where(low, gx, nx - 1 - gx)

    orders = [plane_order(nx, k) for k in range(half)]
    px_of = []
    for m in range(nx):
        q = jnp.int32(orders[0][m])
        for k in range(1, half):
            q = jnp.where(u == k, orders[k][m], q)
        px_of.append(jnp.where(low, q, nx - 1 - q))

    def flip(v, n, j):
        y, b = 0, 1
        while b < n:
            y += lax.rem(v // b + j // b, 2) * b
            b *= 2
        return y

    py_of = [flip(gy, ny, j) for j in range(ny)]

    def span_of(m, first, last):
        return range(max(first, 1) if m == 1 else first, min(last, ny))

    def remote(src, dst, recv_sem, px, py):
        return pltpu.make_async_remote_copy(
            src_ref=src, dst_ref=dst, send_sem=sent, recv_sem=recv_sem,
            device_id=(px, py), device_id_type=MESH)

    def arrived(ref, sem):
        pltpu.make_async_copy(ref, ref, sem).wait()

    small = [pltpu.make_async_copy(src, dst, load_sem.at[n]) for n, src, dst in (
        (0, rows_hbm, rows_ref), (1, hot_rows_hbm, hot_rows_ref),
        (2, bags_hbm, bags_ref), (3, hot_ids_hbm, hot_ids_ref))]
    small[0].start()
    small[1].start()

    barrier = pltpu.get_barrier_semaphore()
    for m in reversed(range(nx)):
        for j in span_of(m, 0, ny):
            pl.semaphore_signal(
                barrier, inc=1, device_id=(px_of[m], py_of[j]), device_id_type=MESH)

    piece = rows_dev // CHUNKS
    for t in range(tcount):
        for c in range(CHUNKS):
            part = pl.ds(c * piece, piece)
            pltpu.make_async_copy(
                tables_ref.at[t, part], tabs[t].at[part], load_sem.at[4 + t]).start()
    small[2].start()
    small[3].start()
    for t in range(tcount):
        tabs[t][rows_dev:rows_dev + PAD, :] = jnp.zeros((PAD, width), jnp.float32)

    small[1].wait()
    local = hot_rows_ref[...] - me * rows_dev
    hot_rows_ref[...] = jnp.where(
        jnp.logical_and(local >= 0, local < rows_dev), local, rows_dev)
    small[0].wait()
    where_hot = pltpu.make_async_copy(hot_rows_ref, hot_at, load_sem.at[1])
    where_hot.start()
    lines = rows_ref[...].reshape(tcount * cap, peers).T
    for p in range(peers):
        idx_out[p, :, 0:tcount * cap] = lines[p:p + 1, :]
    own_idx = pltpu.make_async_copy(idx_out.at[me], idx_s.at[me], load_sem.at[0])
    own_idx.start()

    group = min(hot, 32)

    def pick_hot(t):
        whole = pl.ds(0, rows_dev)
        arrived(tabs[t].at[whole], load_sem.at[4 + t])

        def step(g, carry):
            for j in range(group):
                hot_stage[pl.ds(t * hot + g * group + j, 1), :] = tabs[t][
                    pl.ds(hot_at[t, g * group + j], 1), :]
            return carry
        lax.fori_loop(0, hot // group, step, 0)

    def table_rows(t):
        return pl.ds(t * hot, hot)

    def pair_send(t):
        remote(hot_stage.at[table_rows(t)], pair_in.at[table_rows(t)], pair_recv.at[t],
               gx, partner).start()

    where_hot.wait()
    pick_hot(0)
    pl.semaphore_wait(barrier, peers - 1)
    for m in range(nx):
        for j in span_of(m, 0, ny):
            remote(idx_out.at[px_of[m] * ny + py_of[j]], idx_s.at[me],
                   idx_recv.at[2 * gx + (j >= COLUMN)], px_of[m], py_of[j]).start()

    @pl.when(jnp.logical_not(hub))
    def _():
        pair_send(0)

    for t in range(1, tcount):
        pick_hot(t)

    def pick(p):
        for t in range(tcount):
            for c in range(cap):
                k = t * cap + c
                stage[p, k:k + 1, :] = tabs[t][pl.ds(idx_s[p, 0, k], 1), :]

    def asked(m, far):
        count = ny - COLUMN if far else len(span_of(m, 0, COLUMN))
        arrived(idx_s.at[pl.ds(0, count)], idx_recv.at[2 * px_of[m] + far])

    def take(m, first, last):
        def step(j, carry):
            pick(px_of[m] * ny + flip(gy, ny, j))
            return carry
        span = span_of(m, first, last)
        lax.fori_loop(span.start, span.stop, step, 0)

    def send(m, first, last):
        for j in span_of(m, first, last):
            remote(stage.at[px_of[m] * ny + py_of[j]], recv.at[me], cold_recv.at[gx],
                   px_of[m], py_of[j]).start()

    def rows_of(t, k):
        return pl.ds(pl.multiple_of(t * hot + k * chunk, chunk), chunk)

    def pair_sum(t):
        rows = table_rows(t)
        arrived(pair_in.at[rows], pair_recv.at[t])
        pair_in[rows, :] = pair_in[rows, :] + hot_stage[rows, :]

    def hot_sends(t):
        for k in range(1, chips):
            to = flip(chip, chips, k)
            remote(pair_in.at[rows_of(t, to)], hot_in.at[t, chip], hot_recv.at[t],
                   gx, 2 * to + core).start()
        hot_in[t, chip] = pair_in[rows_of(t, chip), :]

    def hot_reduce(t):
        others = pl.ds(0, chips - 1)
        arrived(hot_in.at[t, others], hot_recv.at[t])
        hot_sum[t, 0] = jnp.sum(hot_in[t], axis=0)

    def z_send(t, k):
        b = 1 << k
        to = gx + b - 2 * b * lax.rem(gx // b, 2)
        remote(hot_sum.at[t, k], hot_z.at[t, k], z_recv.at[t * levels + k], to, gy).start()

    def z_sum(t, k):
        arrived(hot_z.at[t, k], z_recv.at[t * levels + k])
        total = hot_sum[t, k] + hot_z[t, k]
        if k + 1 < levels:
            hot_sum[t, k + 1] = total
        else:
            hot_tab[rows_of(t, chip), :] = total

    def gat_sends(t):
        mine = hot_tab.at[rows_of(t, chip)]
        for k in range(1, chips):
            remote(mine, mine, pair_recv.at[t], gx, 2 * flip(chip, chips, k) + 1 - t % 2).start()
        remote(mine, mine, pair_recv.at[1 - core], gx, partner).start()

    def forward(t):
        apart = pl.ds(0, (chips - 1) * chunk)
        arrived(hot_tab.at[apart], pair_recv.at[t])
        for k in range(1, chips):
            got = hot_tab.at[rows_of(t, flip(chip, chips, k))]
            remote(got, got, pair_recv.at[1 - core], gx, partner).start()

    slots = peers * cap
    owner = lax.broadcasted_iota(jnp.int32, (peers, slots), 1) // cap
    spread = (owner == lax.broadcasted_iota(jnp.int32, (peers, slots), 0)).astype(jnp.float32)
    place = lax.rem(lax.broadcasted_iota(jnp.int32, (cap, slots), 1), cap)
    mask = place == lax.broadcasted_iota(jnp.int32, (cap, slots), 0)
    samples = lax.broadcasted_iota(jnp.int32, (batch, slots), 0).astype(jnp.float32)

    def cold_weights(t):
        wide = jnp.dot(bags_ref[t].astype(jnp.float32), spread,
                       precision=lax.Precision.HIGHEST, preferred_element_type=jnp.float32)
        flat = jnp.sum(jnp.where(mask, wide, 0.0), axis=0, keepdims=True)
        onehot[t] = (flat == samples).astype(jnp.bfloat16)

    entry = lax.broadcasted_iota(jnp.int32, (hot, batch), 0)

    def hot_counts(t):
        total = jnp.zeros((hot, batch), jnp.float32)
        for k in range(hot_ids_ref.shape[1]):
            total += (hot_ids_ref[t, k:k + 1, :] == entry).astype(jnp.float32)
        counts[t] = total.T.astype(jnp.bfloat16)

    tables = range(tcount)
    sums = [jnp.zeros((batch, width), jnp.float32) for _ in tables]

    def pool_plane(m):
        arrived(recv.at[pl.ds(0, len(span_of(m, 0, ny)))], cold_recv.at[px_of[m]])
        at = pl.ds(pl.multiple_of(px_of[m] * ny, ny), ny)
        cols = pl.ds(pl.multiple_of(px_of[m] * ny * cap, ny * cap), ny * cap)
        for t in tables:
            values = recv[at, t * cap:(t + 1) * cap, :].reshape(ny * cap, width)
            sums[t] = sums[t] + pool(onehot[t, :, cols], values)

    def pool_hot():
        for t in tables:
            sums[t] = sums[t] + pool(counts[t], hot_tab[t * hot:(t + 1) * hot, :])

    @pl.when(hub)
    def _():
        pair_sum(0)
        small[2].wait()
        small[3].wait()
        hot_counts(0)
        hot_sends(0)
        for m in (0, *range(3, nx)):
            asked(m, 0)
            take(m, 0, COLUMN)
            send(m, 0, COLUMN)
        for t in range(1, tcount):
            pair_sum(t)
        asked(1, 0)
        take(1, 0, COLUMN)
        for t in range(1, tcount):
            hot_sends(t)
        asked(2, 0)
        take(2, 0, COLUMN)
        send(2, 0, COLUMN)
        for m in (0, *range(3, nx)):
            asked(m, 1)
            take(m, COLUMN, ny)
        asked(1, 1)
        take(1, COLUMN, ny)
        hot_reduce(0)
        asked(2, 1)
        take(2, COLUMN, ny)
        z_send(0, 0)
        for t in range(1, tcount):
            hot_reduce(t)
        own_idx.wait()
        pick(me)
        recv[me] = stage[me]
        for t in range(1, tcount):
            z_send(t, 0)
        for k in range(1, levels):
            for t in tables:
                z_sum(t, k - 1)
                if k == 1 and t == 1:
                    send(1, 0, ny)
                if k == 1 and t == 0:
                    for other in range(1, tcount):
                        hot_counts(other)
                z_send(t, k)
        for a in reversed(range(COLUMN, ny, 2)):
            send(2, a, a + 2)
        for a in reversed(range(COLUMN, ny)):
            for m in (*range(3, nx), 0):
                send(m, a, a + 1)
        for t in tables:
            z_sum(t, levels - 1)
            cold_weights(t)
            gat_sends(t)
        for t in range(0, tcount, 2):
            forward(t)

    @pl.when(jnp.logical_not(hub))
    def _():
        for t in range(1, tcount):
            pair_send(t)
        for m in (0, *range(3, nx)):
            asked(m, 0)
            take(m, 0, COLUMN)
            send(m, 0, COLUMN)
        for a in reversed(range(COLUMN, ny)):
            for m in (0, *range(3, nx)):
                asked(m, 1) if a + 1 == ny else None
                take(m, a, a + 1)
                send(m, a, a + 1)
        asked(2, 0)
        asked(2, 1)
        take(2, 0, ny)
        send(2, 0, ny)
        asked(1, 0)
        asked(1, 1)
        take(1, 0, ny)
        own_idx.wait()
        pick(me)
        send(1, 0, ny)
        recv[me] = stage[me]
        small[2].wait()
        small[3].wait()
        for t in tables:
            hot_counts(t)
            cold_weights(t)

    pool_plane(1)
    pool_plane(2)

    @pl.when(jnp.logical_not(hub))
    def _():
        for t in range(1, tcount, 2):
            forward(t)

    odds = tcount // 2 * (chips - 1)
    evens = tcount + (tcount - tcount // 2) * (chips - 1)

    @pl.when(hub)
    def _():
        arrived(hot_tab.at[pl.ds(0, odds * chunk)], pair_recv.at[1])

    @pl.when(jnp.logical_not(hub))
    def _():
        arrived(hot_tab.at[pl.ds(0, evens * chunk)], pair_recv.at[0])

    pool_hot()
    for m in (*range(3, nx), 0):
        pool_plane(m)
    for t in tables:
        out_ref[t::tcount, :] = sums[t]

    lines_sent = (peers - 1) * (idx_out.shape[2] // width + tcount * cap)
    odd = tcount // 2
    hub_sent = chunk * (tcount * (2 * (chips - 1) + levels + 1) + (tcount - odd) * (chips - 1))
    spoke_sent = tcount * hot + odd * (chips - 1) * chunk

    @pl.when(hub)
    def _():
        arrived(tabs[0].at[pl.ds(0, lines_sent + hub_sent)], sent)

    @pl.when(jnp.logical_not(hub))
    def _():
        arrived(tabs[0].at[pl.ds(0, lines_sent + spoke_sent)], sent)


def solution(mesh):
    nx, ny = mesh.shape["gx"], mesh.shape["gy"]
    peers = nx * ny

    def body(tables, cold_rows, cold_bags, hot_rows, hot_ids):
        tcount, rows_dev, width = tables.shape
        cap = cold_rows.shape[3]
        batch = hot_ids.shape[0]
        hot = hot_rows.shape[1]
        chips = ny // 2
        chunk = hot // chips
        levels = nx.bit_length() - 1
        lanes = -(-tcount * cap // width) * width
        assert nx == 1 << levels and ny & (ny - 1) == 0 and min(nx, ny) > 1
        assert chunk * chips == hot and chunk % 8 == 0 and ny * cap % 128 == 0
        assert tcount == 2 and rows_dev % CHUNKS == 0 and hot & (hot - 1) == 0
        rows_t = jnp.transpose(cold_rows[0], (0, 2, 1))
        bags_t = jnp.transpose(cold_bags[0], (0, 2, 1))
        ids_t = jnp.transpose(hot_ids, (1, 2, 0))
        hbm = pl.BlockSpec(memory_space=pltpu.HBM)
        f32, sem = jnp.float32, pltpu.SemaphoreType.DMA
        out = pl.pallas_call(
            functools.partial(kernel, nx, ny),
            out_shape=pltpu.VMEM((batch * tcount, width), f32),
            in_specs=[hbm] * 5,
            out_specs=pl.BlockSpec(memory_space=pltpu.VMEM),
            scratch_shapes=[
                pltpu.VMEM(rows_t.shape, jnp.int32),
                pltpu.VMEM(bags_t.shape, jnp.int32),
                pltpu.VMEM(hot_rows.shape, jnp.int32),
                pltpu.SMEM(hot_rows.shape, jnp.int32),
                pltpu.VMEM(ids_t.shape, jnp.int32),
                pltpu.VMEM((peers, 1, lanes), jnp.int32),
                pltpu.SMEM((peers, 1, lanes), jnp.int32),
                pltpu.VMEM((peers, tcount * cap, width), f32),
                pltpu.VMEM((peers, tcount * cap, width), f32),
                pltpu.VMEM((tcount * hot, width), f32),
                pltpu.VMEM((tcount * hot, width), f32),
                pltpu.VMEM((tcount, chips, chunk, width), f32),
                pltpu.VMEM((tcount, levels, chunk, width), f32),
                pltpu.VMEM((tcount, levels, chunk, width), f32),
                pltpu.VMEM((tcount * hot, width), f32),
                pltpu.VMEM((tcount, batch, peers * cap), jnp.bfloat16),
                pltpu.VMEM((tcount, batch, hot), jnp.bfloat16),
                sem((4 + tcount,)),
                sem,
                sem((2 * nx,)),
                sem((nx,)),
                sem((tcount,)),
                sem((tcount,)),
                sem((tcount * levels,)),
            ] + [pltpu.VMEM((rows_dev + PAD, width), f32)] * tcount,
            compiler_params=pltpu.CompilerParams(
                collective_id=0, has_side_effects=True,
                vmem_limit_bytes=VMEM_BYTES - 4 * batch * tcount * width),
        )(tables, rows_t, bags_t, hot_rows, ids_t)
        return out.reshape(batch, tcount, width)

    return jax.shard_map(
        body,
        mesh=mesh,
        in_specs=(
            P(None, ("gx", "gy"), None),
            P(("gx", "gy"), None, None, None),
            P(("gx", "gy"), None, None, None),
            P(),
            P(("gx", "gy"), None, None),
        ),
        out_specs=P(("gx", "gy"), None, None),
        check_vma=False,
    )
```
